128 devices in a mesh: seq: 16 (over y, z_lo, core), tensor: 8 (over z_hi, x).
Axes of the slice: x: 4, y: 4, z: 4 (z_hi: 2, z_lo: 2; z = z_hi * 2 + z_lo), core: 2. Of those that a mesh axis runs over, the one named last changes fastest.
Arguments:
- tokens: bfloat16 [8192, 8192], P('seq', 'tensor'), may hold values from -6 to 6
- positions: int32 [8192], P('seq'), may hold values from 0 to 8191, each once
- norm_gain: float32 [8192], replicated, may hold values from 0.1 to 1.9
- w_query: bfloat16 [8192, 4096], P('seq', 'tensor'), may hold values from -0.0625 to 0.0625
- w_key: bfloat16 [8192, 1024], P('seq', 'tensor'), may hold values from -0.0625 to 0.0625
- w_value: bfloat16 [8192, 1024], P('seq', 'tensor'), may hold values from -0.0625 to 0.0625
- b_query: float32 [4096], P('tensor'), may hold values from -40 to 40
- b_key: float32 [1024], P('tensor'), may hold values from -40 to 40
- b_value: float32 [1024], P('tensor'), may hold values from -6 to 6
- w_out: bfloat16 [4096, 8192], P('tensor', 'seq'), may hold values from -0.09375 to 0.09375
Outputs:
- mixed: bfloat16 [8192, 8192], P('seq', 'tensor')
- context: bfloat16 [8192, 4096], P('seq', 'tensor')
The draws below stay inside these ranges and needn't reach their ends.
Inputs may be any that keep to these rules, and one draw needn't show every extreme that they name: positions holds every position 0 to 8191 once.
All inputs are finite; a program needn't handle non-finite values.
Results may differ from the reference program's by a relative error of at most 0.025.
Values may be sent and summed in bfloat16 or wider, within the bound.
A program may use at most 128 MiB of HBM per device.

```python
import jax
import jax.numpy as jnp
from jax import lax

D = 8192
HEADS = 32
KV_HEADS = 8
HD = 128
TOKENS = 8192


def draw_b_query(key, part):
    return jax.random.normal(jax.random.fold_in(key, 14), (HEADS * HD,), jnp.float32)


def draw_b_key(key, part):
    return jax.random.normal(jax.random.fold_in(key, 15), (KV_HEADS * HD,), jnp.float32)


def steps_of(rng, dims, cuts, low, high):
    factor_of, own = 1.0, jax.random.fold_in(rng, 6)
    for position, parts in cuts:
        steps = jnp.exp(jax.random.uniform(jax.random.fold_in(own, position), (parts,), jnp.float32, low / len(cuts), high / len(cuts)))
        factor_of = factor_of * jnp.repeat(steps, dims[position] // parts).reshape([-1 if axis == position else 1 for axis in range(len(dims))])
    return factor_of


def centred(own_key, dims, deviation, bound, split=(), held_as=jnp.bfloat16):
    loudness = steps_of(own_key, dims, split, -0.22, 0.18) if split else 1.0
    array = jax.random.normal(own_key, dims, jnp.float32) * deviation * loudness
    return jnp.minimum(jnp.maximum(array, -bound), bound).astype(held_as)


def setup_inputs(seed: int = 0) -> dict:
    splits = jax.random.split(jax.random.key(seed), 11)
    tokens = centred(splits[0], (TOKENS, D), 1.0, 6.0, ((0, 16), (1, 8)))
    positions = jax.random.permutation(splits[1], TOKENS).astype(jnp.int32)
    norm_gain = jnp.clip(1.0 + 0.18 * jax.random.normal(splits[2], (D,), jnp.float32), 0.1, 1.9)
    w_query = centred(splits[3], (D, HEADS * HD), D ** -0.5, 0.0625, ((0, 16), (1, 8)))
    w_key = centred(splits[4], (D, KV_HEADS * HD), D ** -0.5, 0.0625, ((0, 16), (1, 8)))
    w_value = centred(splits[5], (D, KV_HEADS * HD), D ** -0.5, 0.0625, ((0, 16), (1, 8)))
    b_query = draw_b_query(jax.random.fold_in(splits[10], 71), 0)
    b_key = draw_b_key(jax.random.fold_in(splits[10], 71), 0)
    b_value = centred(splits[8], (KV_HEADS * HD,), 1.0, 6.0, ((0, 8),), jnp.float32)
    w_out = centred(splits[9], (HEADS * HD, D), (HEADS * HD) ** -0.5, 0.09375, ((0, 8), (1, 16)))
    return dict(tokens=tokens, positions=positions, norm_gain=norm_gain, w_query=w_query, w_key=w_key, w_value=w_value, b_query=b_query, b_key=b_key, b_value=b_value, w_out=w_out)


NORM_EPS = 1e-06
ROPE_BASE = 1000000.0
NEG_FILL = -1e+30

def rotate(values_in, positions):
    half_dim = HD // 2
    inv_freq = ROPE_BASE ** (-jnp.arange(half_dim, dtype=jnp.float32) * 2.0 / HD)
    angles = positions.astype(jnp.float32)[:, None] * inv_freq[None, :]
    cosine = jnp.cos(angles)[:, None, :]
    sines = jnp.sin(angles)[:, None, :]
    lower_half = values_in[..., :half_dim]
    upper_half = values_in[..., half_dim:]
    return jnp.concatenate([lower_half * cosine - upper_half * sines, upper_half * cosine + lower_half * sines], -1)

def reference(tokens, positions, norm_gain, w_query, w_key, w_value, b_query, b_key, b_value, w_out):
    group = HEADS // KV_HEADS
    inputs = tokens.astype(jnp.float32)
    inverse_rms = lax.rsqrt(lax.optimization_barrier(jnp.mean(inputs * inputs, -1, keepdims=True)) + NORM_EPS)
    normed = (inputs * inverse_rms * norm_gain.astype(jnp.float32)[None, :]).astype(jnp.bfloat16)
    q_proj = jnp.dot(normed, w_query, preferred_element_type=jnp.float32) + b_query.astype(jnp.float32)[None, :]
    k_proj = jnp.dot(normed, w_key, preferred_element_type=jnp.float32) + b_key.astype(jnp.float32)[None, :]
    v_proj = jnp.dot(normed, w_value, preferred_element_type=jnp.float32) + b_value.astype(jnp.float32)[None, :]
    queries = rotate(q_proj.reshape(TOKENS, HEADS, HD), positions).astype(jnp.bfloat16)
    keys_rot = rotate(k_proj.reshape(TOKENS, KV_HEADS, HD), positions).astype(jnp.bfloat16)
    values = v_proj.astype(jnp.bfloat16).reshape(TOKENS, KV_HEADS, HD)
    queries = jnp.moveaxis(queries, 1, 0)
    keys_rot = jnp.moveaxis(keys_rot, 1, 0)
    values = jnp.moveaxis(values, 1, 0)
    allowed = positions[None, :] <= positions[:, None]
    scale = HD ** (-0.5)

    def one_head(head_index):
        q_head = lax.dynamic_index_in_dim(queries, head_index, 0, keepdims=False).astype(jnp.float32)
        kv_index = head_index // group
        k_head = lax.dynamic_index_in_dim(keys_rot, kv_index, 0, keepdims=False).astype(jnp.float32)
        v_head = lax.dynamic_index_in_dim(values, kv_index, 0, keepdims=False)
        scores = jnp.dot(q_head, k_head.T) * scale
        scores = jnp.where(allowed, scores, NEG_FILL)
        row_max = lax.optimization_barrier(jnp.max(scores, -1, keepdims=True))
        weights = jnp.where(allowed, jnp.exp(scores - row_max), 0.0)
        denominator = lax.optimization_barrier(jnp.sum(weights, -1, keepdims=True))
        numerator = jnp.dot(weights.astype(jnp.bfloat16), v_head, preferred_element_type=jnp.float32)
        return (numerator / denominator).astype(jnp.bfloat16)
    per_head = lax.map(one_head, jnp.arange(HEADS, dtype=jnp.int32))
    context = jnp.moveaxis(per_head, 0, 1).reshape(TOKENS, HEADS * HD)
    mixed = (inputs + jnp.dot(context, w_out, preferred_element_type=jnp.float32)).astype(jnp.bfloat16)
    return (mixed, context)
```

```python
import functools
import math

import jax
import jax.numpy as jnp
from jax import lax
from jax.experimental import pallas as pl
from jax.experimental.pallas import tpu as pltpu
from jax.sharding import PartitionSpec as P

HD = 128
NORM_EPS = 1e-06
ROPE_BASE = 1000000.0
NEG_FILL = -1e30
MESH = pl.DeviceIdType.MESH
BF16 = jnp.bfloat16
F32 = jnp.float32


def coords():
    s, t = lax.axis_index("seq"), lax.axis_index("tensor")
    return dict(y=s // 4, zl=(s // 2) % 2, c=s % 2, zh=t // 4, x=t % 4)


SIZES = dict(y=4, zl=2, c=2, zh=2, x=4)


def moved(k, **shift):
    k = dict(k)
    for name, by in shift.items():
        k[name] = (k[name] + (by + SIZES[name])) % SIZES[name]
    return k


def seq_of(k):
    return k["y"] * 4 + k["zl"] * 2 + k["c"]


def tensor_of(k):
    return k["zh"] * 4 + k["x"]


def device(k):
    return (seq_of(k), tensor_of(k))


class Gather:
    def __init__(self, k, slot, half_rows, ring, pair, sibling, ssem, rsem, base=0):
        self.k, self.slot, self.half = k, slot, half_rows
        self.ring, self.pair, self.sibling = ring, pair, sibling
        self.ssem, self.rsem, self.base = ssem, rsem, base
        self.sent = []

    def at(self, r=0, p=0, c=0):
        return (r, p, c)

    def place(self, where):
        r, p, c = where
        return moved(self.k, **{self.ring: r, self.pair: p, "c": c})

    def copy(self, i, block, target, half):
        ref = self.slot(self.place(block))
        if half is not None:
            ref = ref.at[pl.ds(half * self.half, self.half)]
        return pltpu.make_async_remote_copy(
            src_ref=ref,
            dst_ref=ref,
            send_sem=self.ssem.at[self.base + i],
            recv_sem=self.rsem.at[self.base + i],
            device_id=device(self.place(target)),
            device_id_type=MESH,
        )

    def send(self, i, block, target, half=None):
        self.copy(i, block, target, half).start()
        self.sent.append((i, block, target, half))

    def recv(self, i, block, half=None):
        self.copy(i, block, (0, 0, 1) if self.sibling else (1, 0, 0), half).wait_recv()

    def share(self, i, block):
        if self.sibling:
            self.send(i, block, self.at(c=1))

    def s0(self):
        own = self.at()
        self.send(0, own, self.at(1))
        self.send(1, own, self.at(-1))
        self.send(2, own, self.at(p=1))
        self.share(3, own)

    def s1(self):
        self.recv(0, self.at(-1))
        self.send(4, self.at(-1), self.at(1), 0)
        self.share(5, self.at(-1))
        self.recv(1, self.at(1))
        self.send(6, self.at(1), self.at(-1), 1)
        self.share(7, self.at(1))

    def s2(self):
        self.recv(2, self.at(p=1))
        self.send(8, self.at(p=1), self.at(1))
        self.send(9, self.at(p=1), self.at(-1))
        self.share(10, self.at(p=1))

    def s3(self):
        self.recv(4, self.at(2), 0)
        self.recv(6, self.at(2), 1)
        self.share(11, self.at(2))
        if not self.sibling:
            self.send(13, self.at(2), self.at(p=1))

    def s4(self):
        self.recv(8, self.at(-1, 1))
        if self.sibling:
            self.send(13, self.at(-1, 1), self.at(1), 0)
        self.share(14, self.at(-1, 1))
        self.recv(9, self.at(1, 1))
        if self.sibling:
            self.send(15, self.at(1, 1), self.at(-1), 1)
        self.share(16, self.at(1, 1))

    def s5(self):
        if self.sibling:
            self.recv(13, self.at(2, 1), 0)
            self.recv(15, self.at(2, 1), 1)
            self.share(17, self.at(2, 1))
        else:
            self.recv(13, self.at(2, 1))

    SHARED = {(0, 0): 3, (-1, 0): 5, (1, 0): 7, (0, 1): 10, (2, 0): 11, (-1, 1): 14, (1, 1): 16, (2, 1): 17}

    def recv_sibling(self, r, p):
        self.recv(self.SHARED[(r, p)], self.at(r, p, 1))

    def finish(self):
        for i, block, target, half in self.sent:
            self.copy(i, block, target, half).wait_send()


ORDER = ((0, 0), (-1, 0), (1, 0), (0, 1), (2, 0), (-1, 1), (1, 1), (2, 1))


def pick(index, values):
    out = values[0]
    for i, v in enumerate(values[1:], 1):
        out = jnp.where(index == i, v, out)
    return out


def greet(k, peers):
    barrier = pltpu.get_barrier_semaphore()
    for p in peers:
        pl.semaphore_signal(barrier, inc=1, device_id=device(p), device_id_type=MESH)
    pl.semaphore_wait(barrier, len(peers))


def tensor_peers(k):
    return [moved(k, x=r, zh=p) for r, p in ORDER[1:]]


def seq_peers(k):
    return [
        moved(k, y=r, zl=p, c=c) for r, p in ORDER for c in (0, 1) if (r, p, c) != (0, 0, 0)
    ]


def as_columns(rows):
    parts = [jnp.broadcast_to(rows[i : i + 1, :], (128, 128)).T for i in range(rows.shape[0])]
    return jnp.concatenate(parts, 0)


def project_kernel(
    tokens, pos, gain, w_query, w_key, w_value, bias, cosine, sine, w_out,
    q_out, kv_out, pos_out, wo_out,
    x_all, w_all, acc, normed, ssq, inverse,
    local_sem, x_ssem, x_rsem, w_ssem, w_rsem, s_ssem, s_rsem, p_ssem, p_rsem, t_ssem, t_rsem,
):
    k = coords()
    me_s, me_t = seq_of(k), tensor_of(k)
    rows = tokens.shape[0]
    qc, kc = w_query.shape[1], w_key.shape[1]
    wrows = w_query.shape[0]

    loads = [
        pltpu.make_async_copy(tokens, x_all.at[me_t], local_sem.at[0]),
        pltpu.make_async_copy(w_query, w_all.at[me_s, :, pl.ds(0, qc)], local_sem.at[1]),
        pltpu.make_async_copy(w_key, w_all.at[me_s, :, pl.ds(qc, kc)], local_sem.at[2]),
        pltpu.make_async_copy(w_value, w_all.at[me_s, :, pl.ds(qc + kc, kc)], local_sem.at[3]),
    ]
    for c in loads:
        c.start()
    pos_out[me_s] = pos[...]

    pair_t, pair_s = me_s // 2, me_t * 2 + k["c"]
    stays = me_t == pair_t
    t_k = dict(y=pair_s // 4, zl=(pair_s // 2) % 2, c=k["c"], zh=pair_t // 4, x=pair_t % 4)
    barrier = pltpu.get_barrier_semaphore()
    peers = tensor_peers(k) + seq_peers(k)
    for p in peers:
        pl.semaphore_signal(barrier, inc=1, device_id=device(p), device_id_type=MESH)

    @pl.when(jnp.logical_not(stays))
    def _():
        pl.semaphore_signal(barrier, inc=1, device_id=(pair_s, pair_t), device_id_type=MESH)

    pl.semaphore_wait(barrier, len(peers) + jnp.where(stays, 0, 1))

    xg = Gather(k, lambda b: x_all.at[tensor_of(b)], rows // 2, "x", "zh", False, x_ssem, x_rsem)
    wg = Gather(k, lambda b: w_all.at[seq_of(b)], wrows // 2, "y", "zl", True, w_ssem, w_rsem)
    for c in loads:
        c.wait()
    xg.s0()
    wg.s0()

    for i in range(rows // 128):
        xb = x_all[me_t, pl.ds(i * 128, 128), :].astype(F32)
        total = jnp.sum(xb * xb, -1, keepdims=True)
        ssq[me_t, i : i + 1, :] = jnp.broadcast_to(total, (128, 128)).T[0:1, :]

    def pos_copy(i, b, target):
        ref = pos_out.at[seq_of(b)]
        return pltpu.make_async_remote_copy(
            ref, ref, p_ssem.at[i], p_rsem.at[i], device_id=device(target), device_id_type=MESH
        )

    s_list = [(r, p, c) for r, p in ORDER for c in (0, 1) if (r, p, c) != (0, 0, 0)]
    for i, (r, p, c) in enumerate(s_list):
        pos_copy(i, k, moved(k, y=r, zl=p, c=c)).start()

    def ssq_copy(i, b, target):
        ref = ssq.at[tensor_of(b)]
        return pltpu.make_async_remote_copy(
            ref, ref, s_ssem.at[i], s_rsem.at[i], device_id=device(target), device_id_type=MESH
        )

    for i, (r, p) in enumerate(ORDER[1:]):
        ssq_copy(i, k, moved(k, x=r, zh=p)).start()

    acc[...] = jnp.zeros_like(acc)

    xg.s1()
    wg.s1()
    wg.s2()

    def move_out():
        return pltpu.make_async_remote_copy(
            w_out, wo_out, t_ssem, t_rsem, device_id=(pair_s, pair_t), device_id_type=MESH
        )

    def keep_out():
        return pltpu.make_async_copy(w_out, wo_out, t_rsem)

    @pl.when(jnp.logical_not(stays))
    def _():
        move_out().start()

    @pl.when(stays)
    def _():
        keep_out().start()

    for i, (r, p) in enumerate(ORDER[1:]):
        ssq_copy(i, moved(k, x=-r, zh=p), k).wait_recv()
    total = ssq[0]
    for i in range(1, 8):
        total = total + ssq[i]
    scale = lax.rsqrt(total / (8 * x_all.shape[2]) + NORM_EPS)
    inverse[...] = as_columns(scale[0 : rows // 128, :])

    wg.s3()
    xg.s2()
    wg.s4()
    xg.s3()
    wg.s5()
    for r, p in ORDER:
        wg.recv_sibling(r, p)

    def block(step, carry):
        @pl.when(step == 5)
        def _():
            xg.recv(8, xg.at(-1, 1))

        @pl.when(step == 6)
        def _():
            xg.recv(9, xg.at(1, 1))

        @pl.when(step == 7)
        def _():
            xg.s5()

        dx = pick(step, [r % 4 for r, _ in ORDER])
        dz = pick(step, [p for _, p in ORDER])
        t = ((k["zh"] + dz) % 2) * 4 + (k["x"] + dx) % 4
        g = gain[t]
        for i in range(rows // 128):
            inv = inverse[pl.ds(i * 128, 128), :]
            for j in range(x_all.shape[2] // 128):
                piece = x_all[t, pl.ds(i * 128, 128), pl.ds(j * 128, 128)].astype(F32)
                normed[pl.ds(i * 128, 128), pl.ds(j * 128, 128)] = (
                    piece * inv * g[:, j * 128 : (j + 1) * 128]
                ).astype(BF16)
        part = jnp.dot(normed[:, 0:wrows], w_all[2 * t], preferred_element_type=F32)
        part = part + jnp.dot(
            normed[:, wrows : 2 * wrows], w_all[2 * t + 1], preferred_element_type=F32
        )
        acc[...] += part
        return carry

    lax.fori_loop(0, 8, block, 0)

    cos, sin = cosine[...], sine[...]
    heads = qc // HD
    for h in range(heads + 1):
        u = acc[:, h * HD : (h + 1) * HD] + bias[:, h * HD : (h + 1) * HD]
        turned = (u * cos + pltpu.roll(u, HD // 2, 1) * sin).astype(BF16)
        if h < heads:
            q_out[h] = turned
        else:
            kv_out[:, 0:HD] = turned
    kv_out[:, HD : 2 * HD] = (acc[:, qc + kc :] + bias[:, qc + kc :]).astype(BF16)

    for i, (r, p, c) in enumerate(s_list):
        pos_copy(i, moved(k, y=-r, zl=p, c=c), k).wait_recv()

    @pl.when(jnp.logical_not(stays))
    def _():
        move_out().wait()

    @pl.when(stays)
    def _():
        keep_out().wait()

    for i, (r, p, c) in enumerate(s_list):
        pos_copy(i, k, moved(k, y=r, zl=p, c=c)).wait_send()
    for i, (r, p) in enumerate(ORDER[1:]):
        ssq_copy(i, k, moved(k, x=r, zh=p)).wait_send()
    xg.finish()
    wg.finish()


QT = 128
CHUNKS = ((0, 2), (2, 1), (3, 1))


def attend_kernel(
    q, kv, pos_all, wo, tokens,
    mixed, context,
    kv_all, wo_all, ctx_all, tok, key_pos, own_pos, top, low, num, mixed_v,
    local_sem, kv_ssem, kv_rsem, wo_ssem, wo_rsem, c_ssem, c_rsem,
):
    k = coords()
    me_s, me_t = seq_of(k), tensor_of(k)
    heads, rows, _ = q.shape
    cw = heads * HD
    wo_load = pltpu.make_async_copy(wo, wo_all.at[pl.ds((me_s // 2) * cw, cw), pl.ds(k["c"] * cw, cw)], local_sem.at[1])
    loads = [
        pltpu.make_async_copy(kv, kv_all.at[pl.ds(me_s * rows, rows)], local_sem.at[0]),
        pltpu.make_async_copy(tokens, tok, local_sem.at[2]),
    ]
    for c in loads:
        c.start()
    wo_load.start()
    greet(k, tensor_peers(k) + seq_peers(k))
    loads[0].wait()

    kg = Gather(
        k, lambda b: kv_all.at[pl.ds(seq_of(b) * rows, rows)], rows // 2, "y", "zl", True, kv_ssem, kv_rsem
    )
    wg = Gather(
        k,
        lambda b: wo_all.at[pl.ds((seq_of(b) // 2) * cw, cw), pl.ds(b["c"] * cw, cw)],
        cw // 2, "y", "zl", True, wo_ssem, wo_rsem,
    )

    def ctx_slot(first, count):
        return lambda b: ctx_all.at[pl.ds(first * QT, count * QT), pl.ds(tensor_of(b) * cw, cw)]

    cg = [
        Gather(k, ctx_slot(f, n), n * QT // 2, "x", "zh", False, c_ssem, c_rsem, base=16 * i)
        for i, (f, n) in enumerate(CHUNKS)
    ]
    kg.s0()

    def spread(s, carry):
        for j in range(rows // 128):
            key_pos[s, :, j * 128 : (j + 1) * 128] = pos_all[s, j : j + 1, :]
        return carry

    lax.fori_loop(0, pos_all.shape[0], spread, 0)
    own_pos[...] = as_columns(pos_all[me_s][0 : rows // 128, :])
    top[...] = jnp.full_like(top, NEG_FILL)
    low[...] = jnp.zeros_like(low)
    num[...] = jnp.zeros_like(num)
    factor = HD ** (-0.5) / math.log(2.0)
    keys = 2 * rows

    events = {}

    def event(step, fn):
        events.setdefault(step, []).append(fn)

    event(0, lambda: kg.recv_sibling(0, 0))
    event(2, lambda: (kg.s1(), kg.s2(), kg.recv_sibling(-1, 0)))
    event(4, lambda: kg.recv_sibling(1, 0))
    event(6, lambda: (kg.recv_sibling(0, 1), kg.s3(), kg.s4(), wo_load.wait(), wg.s0()))
    event(8, lambda: kg.recv_sibling(2, 0))
    event(10, lambda: kg.recv_sibling(-1, 1))
    event(12, lambda: (kg.recv_sibling(1, 1), kg.s5()))
    event(14, lambda: kg.recv_sibling(2, 1))
    event(19, lambda: (wg.s1(), wg.s2()))
    event(28, lambda: (wg.s3(), wg.s4()))

    total_steps = 8 * (rows // QT)
    done_at = []
    at = 0
    for f, n in CHUNKS:
        at += 8 * n
        done_at.append(at)

    def close(i):
        f, n = CHUNKS[i]
        r = pl.ds(f * QT, n * QT)
        for h in range(heads):
            bottom = jnp.sum(low[h, r, :], -1, keepdims=True)
            ctx_all[r, pl.ds(pl.multiple_of(me_t * cw + h * HD, HD), HD)] = (num[h, r, :] / bottom).astype(BF16)

    def step(g, carry):
        for at, fns in sorted(events.items()):
            @pl.when(g == at)
            def _(fns=fns):
                for fn in fns:
                    fn()

        first = g < 16
        kb = jnp.where(first, g // 2, g % 8)
        tile = jnp.where(first, g % 2, g // 8)
        dy = pick(kb, [r % 4 for r, _ in ORDER])
        dz = pick(kb, [p for _, p in ORDER])
        block = ((k["y"] + dy) % 4) * 2 + (k["zl"] + dz) % 2
        kr = pl.ds(pl.multiple_of(block * keys, keys), keys)
        qr = pl.ds(pl.multiple_of(tile * QT, QT), QT)
        mine = own_pos[qr, :]

        def head(h, c):
            s = lax.dot_general(
                q[h, qr, :], kv_all[kr, 0:HD], (((1,), (1,)), ((), ())), preferred_element_type=F32
            )
            parts = []
            for j in range(keys // 128):
                kp = key_pos[block * 2 + j // (rows // 128), :, (j % (rows // 128)) * 128 : (j % (rows // 128) + 1) * 128]
                parts.append(jnp.where(kp <= mine, s[:, j * 128 : (j + 1) * 128], NEG_FILL))
            best = parts[0]
            for x in parts[1:]:
                best = jnp.maximum(best, x)
            old = top[h, qr, :]
            new = jnp.maximum(old, jnp.max(best, -1, keepdims=True))
            top[h, qr, :] = new
            alpha = jnp.exp2((old - new) * factor)
            weights, total = [], low[h, qr, :] * alpha
            for x in parts:
                w = jnp.exp2((x - new) * factor)
                total = total + w
                weights.append(w.astype(BF16))
            low[h, qr, :] = total
            num[h, qr, :] = num[h, qr, :] * alpha + jnp.dot(
                jnp.concatenate(weights, 1), kv_all[kr, HD : 2 * HD], preferred_element_type=F32
            )
            return c

        lax.fori_loop(0, heads, head, 0)
        return carry

    for i in range(len(CHUNKS) - 1):
        event(done_at[i], functools.partial(lambda i: (close(i), cg[i].s0()), i))
    event(26, lambda: (cg[0].s1(), cg[0].s2()))
    event(30, lambda: cg[0].s3())
    lax.fori_loop(0, total_steps, step, 0)

    last = len(CHUNKS) - 1
    close(last)
    cg[last].s0()
    put = pltpu.make_async_copy(ctx_all.at[:, pl.ds(pl.multiple_of(me_t * cw, cw), cw)], context, local_sem.at[3])
    put.start()
    for i in range(1, last + 1):
        cg[i].s1()
        cg[i].s2()
        if i == 1:
            wg.s5()
        cg[i].s3()
    for r, p in ORDER:
        wg.recv_sibling(r, p)
    loads[1].wait()

    def output(i):
        f, n = CHUNKS[i]
        for m in range(n):
            r = pl.ds((f + m) * QT, QT)

            def half(c, carry):
                cols = pl.ds(pl.multiple_of(c * 256, 256), 256)
                summed = jnp.dot(ctx_all[r, :], wo_all[:, cols], preferred_element_type=F32)
                mixed_v[r, cols] = (tok[r, cols].astype(F32) + summed).astype(BF16)
                return carry

            lax.fori_loop(0, tok.shape[1] // 256, half, 0)

    puts = []
    for i in range(last + 1):
        cg[i].s4()
        cg[i].s5()
        output(i)
        f, n = CHUNKS[i]
        r = pl.ds(f * QT, n * QT)
        c = pltpu.make_async_copy(mixed_v.at[r], mixed.at[r], local_sem.at[4 + i])
        c.start()
        puts.append(c)
    put.wait()
    for c in puts:
        c.wait()
    kg.finish()
    wg.finish()
    for x in cg:
        x.finish()


def shards(tokens, positions, norm_gain, w_query, w_key, w_value, b_query, b_key, b_value, w_out):
    rows, feats = tokens.shape
    qc, kc = w_query.shape[1], w_key.shape[1]
    wrows = w_query.shape[0]
    heads = qc // HD
    nt, ns = lax.axis_size("tensor"), lax.axis_size("seq")
    half = HD // 2
    inv_freq = ROPE_BASE ** (-jnp.arange(half, dtype=F32) * 2.0 / HD)
    angles = positions.astype(F32)[:, None] * inv_freq[None, :]
    cos, sin = jnp.cos(angles), jnp.sin(angles)
    cosine = jnp.concatenate([cos, cos], 1)
    sine = jnp.concatenate([-sin, sin], 1)
    bias = jnp.concatenate((b_query, b_key, b_value))[None, :]
    pos = jnp.pad(positions.astype(F32).reshape(rows // 128, 128), ((0, 8 - rows // 128), (0, 0)))
    any_, vmem = pl.BlockSpec(memory_space=pl.ANY), pl.BlockSpec(memory_space=pltpu.VMEM)
    dma = pltpu.SemaphoreType.DMA
    q, kv, pos_all, wo = pl.pallas_call(
        project_kernel,
        name="project",
        out_shape=(
            jax.ShapeDtypeStruct((heads, rows, HD), BF16),
            jax.ShapeDtypeStruct((rows, 2 * HD), BF16),
            jax.ShapeDtypeStruct((ns, 8, 128), F32),
            jax.ShapeDtypeStruct(w_out.shape, BF16),
        ),
        in_specs=[any_, vmem, vmem, any_, any_, any_, vmem, vmem, vmem, any_],
        out_specs=(vmem, vmem, vmem, any_),
        scratch_shapes=[
            pltpu.VMEM((nt, rows, feats), BF16),
            pltpu.VMEM((ns, wrows, qc + 2 * kc), BF16),
            pltpu.VMEM((rows, qc + 2 * kc), F32),
            pltpu.VMEM((rows, feats), BF16),
            pltpu.VMEM((nt, 8, 128), F32),
            pltpu.VMEM((rows, 128), F32),
            dma((4,)), dma((20,)), dma((20,)), dma((20,)), dma((20,)),
            dma((8,)), dma((8,)), dma((16,)), dma((16,)), dma, dma,
        ],
        compiler_params=pltpu.CompilerParams(
            collective_id=0, has_side_effects=True, vmem_limit_bytes=48 * 1024 * 1024
        ),
    )(tokens, pos, norm_gain.reshape(nt, 1, feats), w_query, w_key, w_value, bias, cosine, sine, w_out)
    mixed, context = pl.pallas_call(
        attend_kernel,
        name="attend",
        out_shape=(
            jax.ShapeDtypeStruct((rows, feats), BF16),
            jax.ShapeDtypeStruct((rows, qc), BF16),
        ),
        in_specs=[vmem, any_, vmem, any_, any_],
        out_specs=(any_, any_),
        scratch_shapes=[
            pltpu.VMEM((ns * rows, 2 * HD), BF16),
            pltpu.VMEM((nt * qc, feats), BF16),
            pltpu.VMEM((rows, nt * qc), BF16),
            pltpu.VMEM((rows, feats), BF16),
            pltpu.VMEM((ns, 1, rows), F32),
            pltpu.VMEM((rows, 128), F32),
            pltpu.VMEM((heads, rows, 128), F32),
            pltpu.VMEM((heads, rows, 128), F32),
            pltpu.VMEM((heads, rows, HD), F32),
            pltpu.VMEM((rows, feats), BF16),
            dma((8,)), dma((20,)), dma((20,)), dma((20,)), dma((20,)), dma((48,)), dma((48,)),
        ],
        compiler_params=pltpu.CompilerParams(
            collective_id=1, has_side_effects=True, vmem_limit_bytes=48 * 1024 * 1024
        ),
    )(q, kv, pos_all, wo, tokens)
    return (mixed, context)


def solution(mesh):
    in_specs = (
        P("seq", "tensor"),
        P("seq"),
        P(),
        P("seq", "tensor"),
        P("seq", "tensor"),
        P("seq", "tensor"),
        P("tensor"),
        P("tensor"),
        P("tensor"),
        P("tensor", "seq"),
    )
    out_specs = (P("seq", "tensor"), P("seq", "tensor"))
    return jax.shard_map(shards, mesh=mesh, in_specs=in_specs, out_specs=out_specs, check_vma=False)
```

```python
import functools
import math

import jax
import jax.numpy as jnp
from jax import lax
from jax.experimental import pallas as pl
from jax.experimental.pallas import tpu as pltpu
from jax.sharding import PartitionSpec as P

HD = 128
NORM_EPS = 1e-06
ROPE_BASE = 1000000.0
NEG_FILL = -1e30
MESH = pl.DeviceIdType.MESH
BF16 = jnp.bfloat16
F32 = jnp.float32


def coords():
    s, t = lax.axis_index("seq"), lax.axis_index("tensor")
    return dict(y=s // 4, zl=(s // 2) % 2, c=s % 2, zh=t // 4, x=t % 4)


SIZES = dict(y=4, zl=2, c=2, zh=2, x=4)


def moved(k, **shift):
    k = dict(k)
    for name, by in shift.items():
        k[name] = (k[name] + (by + SIZES[name])) % SIZES[name]
    return k


def seq_of(k):
    return k["y"] * 4 + k["zl"] * 2 + k["c"]


def tensor_of(k):
    return k["zh"] * 4 + k["x"]


def device(k):
    return (seq_of(k), tensor_of(k))


class Gather:
    def __init__(self, k, slot, half_rows, ring, pair, sibling, ssem, rsem, base=0):
        self.k, self.slot, self.half = k, slot, half_rows
        self.ring, self.pair, self.sibling = ring, pair, sibling
        self.ssem, self.rsem, self.base = ssem, rsem, base
        self.sent = []

    def at(self, r=0, p=0, c=0):
        return (r, p, c)

    def place(self, where):
        r, p, c = where
        return moved(self.k, **{self.ring: r, self.pair: p, "c": c})

    def copy(self, i, block, target, half):
        ref = self.slot(self.place(block))
        if half is not None:
            ref = ref.at[pl.ds(half * self.half, self.half)]
        return pltpu.make_async_remote_copy(
            src_ref=ref,
            dst_ref=ref,
            send_sem=self.ssem.at[self.base + i],
            recv_sem=self.rsem.at[self.base + i],
            device_id=device(self.place(target)),
            device_id_type=MESH,
        )

    def send(self, i, block, target, half=None):
        self.copy(i, block, target, half).start()
        self.sent.append((i, block, target, half))

    def recv(self, i, block, half=None):
        self.copy(i, block, (0, 0, 1) if self.sibling else (1, 0, 0), half).wait_recv()

    def share(self, i, block):
        if self.sibling:
            self.send(i, block, self.at(c=1))

    def s0(self):
        own = self.at()
        self.send(0, own, self.at(1))
        self.send(1, own, self.at(-1))
        if self.sibling:
            self.send(2, own, self.at(p=1))
        self.share(3, own)

    def pair_halves(self):
        self.send(2, self.at(), self.at(p=1), 0)
        self.send(3, self.at(), self.at(p=1), 1)

    def s1(self):
        self.recv(0, self.at(-1))
        self.send(4, self.at(-1), self.at(1), 0)
        self.share(5, self.at(-1))
        self.recv(1, self.at(1))
        self.send(6, self.at(1), self.at(-1), 1)
        self.share(7, self.at(1))

    def s2(self):
        self.recv(2, self.at(p=1))
        self.send(8, self.at(p=1), self.at(1))
        self.send(9, self.at(p=1), self.at(-1))
        self.share(10, self.at(p=1))

    def s2_half(self, h):
        self.recv(2 + h, self.at(p=1), h)
        self.send(8 + 2 * h, self.at(p=1), self.at(1), h)
        self.send(9 + 2 * h, self.at(p=1), self.at(-1), h)

    def s4_halves(self):
        for h in (0, 1):
            self.recv(8 + 2 * h, self.at(-1, 1), h)
            self.recv(9 + 2 * h, self.at(1, 1), h)

    def s3(self):
        self.recv(4, self.at(2), 0)
        self.recv(6, self.at(2), 1)
        self.share(11, self.at(2))
        if not self.sibling:
            self.send(13, self.at(2), self.at(p=1))

    def s4(self):
        self.recv(8, self.at(-1, 1))
        if self.sibling:
            self.send(13, self.at(-1, 1), self.at(1), 0)
        self.share(14, self.at(-1, 1))
        self.recv(9, self.at(1, 1))
        if self.sibling:
            self.send(15, self.at(1, 1), self.at(-1), 1)
        self.share(16, self.at(1, 1))

    def s5(self):
        if self.sibling:
            self.recv(13, self.at(2, 1), 0)
            self.recv(15, self.at(2, 1), 1)
            self.share(17, self.at(2, 1))
        else:
            self.recv(13, self.at(2, 1))

    SHARED = {(0, 0): 3, (-1, 0): 5, (1, 0): 7, (0, 1): 10, (2, 0): 11, (-1, 1): 14, (1, 1): 16, (2, 1): 17}

    def recv_sibling(self, r, p):
        self.recv(self.SHARED[(r, p)], self.at(r, p, 1))

    def finish(self):
        for i, block, target, half in self.sent:
            self.copy(i, block, target, half).wait_send()


ORDER = ((0, 0), (-1, 0), (1, 0), (0, 1), (2, 0), (-1, 1), (1, 1), (2, 1))


def pick(index, values):
    out = values[0]
    for i, v in enumerate(values[1:], 1):
        out = jnp.where(index == i, v, out)
    return out


def greet(k, peers):
    barrier = pltpu.get_barrier_semaphore()
    for p in peers:
        pl.semaphore_signal(barrier, inc=1, device_id=device(p), device_id_type=MESH)
    pl.semaphore_wait(barrier, len(peers))


def tensor_peers(k):
    return [moved(k, x=r, zh=p) for r, p in ORDER[1:]]


def seq_peers(k):
    return [
        moved(k, y=r, zl=p, c=c) for r, p in ORDER for c in (0, 1) if (r, p, c) != (0, 0, 0)
    ]


def as_columns(rows):
    parts = [jnp.broadcast_to(rows[i : i + 1, :], (128, 128)).T for i in range(rows.shape[0])]
    return jnp.concatenate(parts, 0)


QT = 128
CHUNKS = ((0, 2), (2, 1), (3, 1))
GROUP = 2


def block_kernel(
    tokens, pos, gain, w_query, w_key, w_value, bias, cosine, sine, w_out,
    mixed, context,
    x_all, w_all, acc, normed, ssq, inverse, wo_mid, pos_all,
    q, kv_all, wo_all, ctx_all, key_pos, own_pos, top, low, num, mixed_v,
    local_sem, x_ssem, x_rsem, w_ssem, w_rsem, s_ssem, s_rsem, p_ssem, p_rsem, t_ssem, t_rsem,
    kv_ssem, kv_rsem, wo_ssem, wo_rsem, c_ssem, c_rsem,
):
    k = coords()
    me_s, me_t = seq_of(k), tensor_of(k)
    rows = tokens.shape[0]
    qc, kc = w_query.shape[1], w_key.shape[1]
    wrows = w_query.shape[0]
    heads = qc // HD
    cw = qc

    loads = [
        pltpu.make_async_copy(tokens, x_all.at[me_t], local_sem.at[0]),
        pltpu.make_async_copy(w_query, w_all.at[me_s, :, pl.ds(0, qc)], local_sem.at[1]),
        pltpu.make_async_copy(w_key, w_all.at[me_s, :, pl.ds(qc, kc)], local_sem.at[2]),
        pltpu.make_async_copy(w_value, w_all.at[me_s, :, pl.ds(qc + kc, kc)], local_sem.at[3]),
        pltpu.make_async_copy(pos, pos_all.at[me_s], local_sem.at[4]),
    ]
    for c in loads:
        c.start()
    greet(k, tensor_peers(k) + seq_peers(k))
    for c in loads:
        c.wait()

    def wo_slot(b):
        return wo_all.at[:, seq_of(b) // 2, :, pl.ds(pl.multiple_of(b["c"] * cw, cw), cw)]

    def ctx_slot(first, count):
        return lambda b: ctx_all.at[
            pl.ds(first * QT, count * QT), pl.ds(pl.multiple_of(tensor_of(b) * cw, cw), cw)
        ]

    xg = Gather(k, lambda b: x_all.at[tensor_of(b)], rows // 2, "x", "zh", False, x_ssem, x_rsem)
    wg = Gather(k, lambda b: w_all.at[seq_of(b)], wrows // 2, "y", "zl", True, w_ssem, w_rsem)
    kg = Gather(
        k, lambda b: kv_all.at[pl.ds(pl.multiple_of(seq_of(b) * rows, rows), rows)], rows // 2,
        "y", "zl", True, kv_ssem, kv_rsem,
    )
    og = Gather(k, wo_slot, wo_all.shape[0] // 2, "y", "zl", True, wo_ssem, wo_rsem)
    cg = [
        Gather(k, ctx_slot(f, n), n * QT // 2, "x", "zh", False, c_ssem, c_rsem, base=16 * i)
        for i, (f, n) in enumerate(CHUNKS)
    ]

    eighth = wo_mid.shape[1]

    def spread_copy(i, source, target):
        return pltpu.make_async_remote_copy(
            w_out.at[pl.ds((seq_of(target) // 2) * eighth, eighth)], wo_mid.at[seq_of(source) // 2],
            t_ssem.at[i], t_rsem.at[i], device_id=device(target), device_id_type=MESH,
        )

    def wo_part(t):
        return wo_all.at[t, me_s // 2, :, pl.ds(pl.multiple_of(k["c"] * cw, cw), cw)]

    def settle_copy(i, source, target):
        return pltpu.make_async_remote_copy(
            wo_mid.at[tensor_of(target)], wo_part(tensor_of(source)),
            t_ssem.at[8 + i], t_rsem.at[8 + i], device_id=device(target), device_id_type=MESH,
        )

    spread_own = pltpu.make_async_copy(
        w_out.at[pl.ds((me_s // 2) * eighth, eighth)], wo_mid.at[me_s // 2], t_ssem.at[7]
    )
    settle_own = pltpu.make_async_copy(wo_mid.at[me_t], wo_part(me_t), t_ssem.at[15])

    def pos_copy(i, b, target):
        ref = pos_all.at[seq_of(b)]
        return pltpu.make_async_remote_copy(
            ref, ref, p_ssem.at[i], p_rsem.at[i], device_id=device(target), device_id_type=MESH
        )

    s_list = [(r, p, c) for r, p in ORDER for c in (0, 1) if (r, p, c) != (0, 0, 0)]

    def ssq_copy(i, b, target):
        ref = ssq.at[tensor_of(b)]
        return pltpu.make_async_remote_copy(
            ref, ref, s_ssem.at[i], s_rsem.at[i], device_id=device(target), device_id_type=MESH
        )

    wg.s0()
    xg.s0()
    for i in range(rows // 128):
        xb = x_all[me_t, pl.ds(i * 128, 128), :].astype(F32)
        total = jnp.sum(xb * xb, -1, keepdims=True)
        ssq[me_t, i : i + 1, :] = jnp.broadcast_to(total, (128, 128)).T[0:1, :]
    for i, (r, p) in enumerate(ORDER[1:]):
        spread_copy(i, k, moved(k, y=r, zl=p)).start()
    spread_own.start()
    for i, (r, p, c) in enumerate(s_list):
        pos_copy(i, k, moved(k, y=r, zl=p, c=c)).start()
    acc[...] = jnp.zeros_like(acc)
    top[...] = jnp.full_like(top, NEG_FILL)
    low[...] = jnp.zeros_like(low)
    num[...] = jnp.zeros_like(num)
    for i, (r, p) in enumerate(ORDER[1:]):
        ssq_copy(i, k, moved(k, x=r, zh=p)).start()

    wg.s1()
    wg.s2()
    xg.pair_halves()
    xg.s1()
    for i, (r, p) in enumerate(ORDER[1:]):
        ssq_copy(i, moved(k, x=-r, zh=p), k).wait_recv()
    total = ssq[0]
    for i in range(1, 8):
        total = total + ssq[i]
    scale = lax.rsqrt(total / (8 * x_all.shape[2]) + NORM_EPS)
    inverse[...] = as_columns(scale[0 : rows // 128, :])
    wg.s3()
    xg.s2_half(0)
    for i, (r, p) in enumerate(ORDER[1:]):
        spread_copy(i, moved(k, y=-r, zl=p), moved(k, y=r, zl=p)).wait_recv()
    spread_own.wait()
    for i, (r, p) in enumerate(ORDER[1:]):
        settle_copy(i, k, moved(k, x=r, zh=p)).start()
    settle_own.start()
    xg.s3()
    xg.s2_half(1)
    wg.s4()
    for i, (r, p, c) in enumerate(s_list):
        pos_copy(i, moved(k, y=-r, zl=p, c=c), k).wait_recv()

    def spread(s, carry):
        for j in range(rows // 128):
            key_pos[s, :, j * 128 : (j + 1) * 128] = pos_all[s, j : j + 1, :]
        return carry

    lax.fori_loop(0, pos_all.shape[0], spread, 0)
    own_pos[...] = as_columns(pos_all[me_s][0 : rows // 128, :])
    for i, (r, p) in enumerate(ORDER[1:]):
        settle_copy(i, moved(k, x=-r, zh=p), moved(k, x=r, zh=p)).wait_recv()
    settle_own.wait()
    og.s0()
    wg.s5()
    for r, p in ORDER:
        wg.recv_sibling(r, p)

    def block(step, carry):
        @pl.when(step == 5)
        def _():
            xg.s4_halves()

        @pl.when(step == 7)
        def _():
            xg.s5()

        dx = pick(step, [r % 4 for r, _ in ORDER])
        dz = pick(step, [p for _, p in ORDER])
        t = ((k["zh"] + dz) % 2) * 4 + (k["x"] + dx) % 4
        g = gain[t]
        for i in range(rows // 128):
            inv = inverse[pl.ds(i * 128, 128), :]
            for j in range(x_all.shape[2] // 128):
                piece = x_all[t, pl.ds(i * 128, 128), pl.ds(j * 128, 128)].astype(F32)
                normed[pl.ds(i * 128, 128), pl.ds(j * 128, 128)] = (
                    piece * inv * g[:, j * 128 : (j + 1) * 128]
                ).astype(BF16)
        part = jnp.dot(normed[:, 0:wrows], w_all[2 * t], preferred_element_type=F32)
        part = part + jnp.dot(
            normed[:, wrows : 2 * wrows], w_all[2 * t + 1], preferred_element_type=F32
        )
        acc[...] += part
        return carry

    lax.fori_loop(0, 8, block, 0)

    cos, sin = cosine[...], sine[...]
    mine_r = pl.ds(pl.multiple_of(me_s * rows, rows), rows)

    def turned(h):
        u = acc[:, h * HD : (h + 1) * HD] + bias[:, h * HD : (h + 1) * HD]
        return (u * cos + pltpu.roll(u, HD // 2, 1) * sin).astype(BF16)

    kv_all[mine_r, 0:HD] = turned(heads)
    kv_all[mine_r, HD : 2 * HD] = (acc[:, qc + kc :] + bias[:, qc + kc :]).astype(BF16)
    for h in range(heads):
        q[h] = turned(h)
    kg.s0()

    factor = HD ** (-0.5) / math.log(2.0)
    keys = 2 * rows
    tiles = rows // QT
    events = {}

    def event(step, *fns):
        events.setdefault(step, []).extend(fns)

    def sib(r, p):
        return lambda: kg.recv_sibling(r, p)

    def close(i):
        f, n = CHUNKS[i]
        r = pl.ds(f * QT, n * QT)
        for h in range(heads):
            bottom = jnp.sum(low[h, r, :], -1, keepdims=True)
            ctx_all[r, pl.ds(pl.multiple_of(me_t * cw + h * HD, HD), HD)] = (
                num[h, r, :] / bottom
            ).astype(BF16)

    def send_ctx(i):
        cg[i].s0()
        cg[i].pair_halves()

    event(0, sib(0, 0))
    event(4, kg.s1, sib(-1, 0))
    event(5, kg.s2)
    event(6, sib(1, 0))
    event(8, sib(0, 1))
    event(10, kg.s3, sib(2, 0))
    event(12, kg.s4, sib(-1, 1), og.s1)
    event(14, sib(1, 1))
    event(16, kg.s5, sib(2, 1), og.s2)
    event(18, lambda: close(0), lambda: send_ctx(0))
    event(24, cg[0].s1)
    event(25, lambda: close(1), lambda: send_ctx(1), lambda: cg[0].s2_half(0))
    event(27, lambda: cg[0].s2_half(1))
    event(29, cg[0].s3, og.s3)

    def step(g, carry):
        for at, fns in sorted(events.items()):
            @pl.when(g == at)
            def _(fns=fns):
                for fn in fns:
                    fn()

        late = jnp.maximum(g - 18, 0)
        mid = jnp.maximum(g - 4, 0)
        kb = jnp.where(g < 4, 0, jnp.where(g < 18, 1 + mid // 2, 1 + late % 7))
        tile = jnp.where(g < 4, g, jnp.where(g < 18, mid % 2, 2 + late // 7))
        dy = pick(kb, [r % 4 for r, _ in ORDER])
        dz = pick(kb, [p for _, p in ORDER])
        chip = ((k["y"] + dy) % 4) * 2 + (k["zl"] + dz) % 2
        kr = pl.ds(pl.multiple_of(chip * keys, keys), keys)
        qr = pl.ds(pl.multiple_of(tile * QT, QT), QT)
        mine = jnp.concatenate([own_pos[qr, :]] * GROUP, 0)
        gr = GROUP * QT

        def scores(u):
            hs = slice(u * GROUP, (u + 1) * GROUP)
            return lax.dot_general(
                q[hs, qr, :].reshape(gr, HD), kv_all[kr, 0:HD], (((1,), (1,)), ((), ())),
                preferred_element_type=F32,
            )

        def soften(u, s):
            hs = slice(u * GROUP, (u + 1) * GROUP)
            parts = []
            for j in range(keys // 128):
                at = (j % (rows // 128)) * 128
                kp = key_pos[chip * 2 + j // (rows // 128), :, at : at + 128]
                parts.append(jnp.where(kp <= mine, s[:, j * 128 : (j + 1) * 128], NEG_FILL))
            best = parts[0]
            for x in parts[1:]:
                best = jnp.maximum(best, x)
            old = top[hs, qr, :].reshape(gr, 128)
            new = jnp.maximum(old, jnp.max(best, -1, keepdims=True))
            top[hs, qr, :] = new.reshape(GROUP, QT, 128)
            alpha = jnp.exp2((old - new) * factor)
            weights, total = [], low[hs, qr, :].reshape(gr, 128) * alpha
            for x in parts:
                w = jnp.exp2((x - new) * factor)
                total = total + w
                weights.append(w.astype(BF16))
            low[hs, qr, :] = total.reshape(GROUP, QT, 128)
            return alpha, jnp.concatenate(weights, 1)

        def collect(u, alpha, weights):
            hs = slice(u * GROUP, (u + 1) * GROUP)
            out = num[hs, qr, :].reshape(gr, HD) * alpha + jnp.dot(
                weights, kv_all[kr, HD : 2 * HD], preferred_element_type=F32
            )
            num[hs, qr, :] = out.reshape(GROUP, QT, HD)

        units = heads // GROUP
        s, held = scores(0), None
        for u in range(units):
            later = scores(u + 1) if u + 1 < units else None
            now = soften(u, s)
            if held is not None:
                collect(u - 1, *held)
            s, held = later, now
        collect(units - 1, *held)
        return carry

    lax.fori_loop(0, 8 * tiles, step, 0)

    close(2)
    send_ctx(2)
    put = pltpu.make_async_copy(
        ctx_all.at[:, pl.ds(pl.multiple_of(me_t * cw, cw), cw)], context, local_sem.at[5]
    )
    put.start()
    cg[1].s1()
    cg[1].s2_half(0)
    cg[1].s2_half(1)
    og.s4()
    cg[1].s3()
    cg[2].s1()
    cg[2].s2_half(0)
    cg[2].s2_half(1)
    cg[2].s3()
    og.s5()
    for r, p in ORDER:
        og.recv_sibling(r, p)

    def output(first, count):
        r = pl.ds(first * QT, count * QT)

        def part(c, carry):
            cols = pl.ds(pl.multiple_of(c * 256, 256), 256)
            w = wo_all[:, :, :, cols].reshape(ctx_all.shape[1], 256)
            summed = jnp.dot(ctx_all[r, :], w, preferred_element_type=F32)
            mixed_v[r, cols] = (x_all[me_t, r, cols].astype(F32) + summed).astype(BF16)
            return carry

        lax.fori_loop(0, mixed_v.shape[1] // 256, part, 0)
        c = pltpu.make_async_copy(mixed_v.at[r], mixed.at[r], local_sem.at[6 + first])
        c.start()
        return c

    cg[0].s4_halves()
    cg[0].s5()
    puts = [put, output(0, 2)]
    for i in (1, 2):
        cg[i].s4_halves()
        cg[i].s5()
    puts.append(output(2, 2))
    for c in puts:
        c.wait()
    for i, (r, p) in enumerate(ORDER[1:]):
        spread_copy(i, k, moved(k, y=r, zl=p)).wait_send()
        settle_copy(i, k, moved(k, x=r, zh=p)).wait_send()
        ssq_copy(i, k, moved(k, x=r, zh=p)).wait_send()
    for i, (r, p, c) in enumerate(s_list):
        pos_copy(i, k, moved(k, y=r, zl=p, c=c)).wait_send()
    for x in [xg, wg, kg, og, *cg]:
        x.finish()


def shards(tokens, positions, norm_gain, w_query, w_key, w_value, b_query, b_key, b_value, w_out):
    rows, feats = tokens.shape
    qc, kc = w_query.shape[1], w_key.shape[1]
    wrows = w_query.shape[0]
    heads = qc // HD
    nt, ns = lax.axis_size("tensor"), lax.axis_size("seq")
    half = HD // 2
    inv_freq = ROPE_BASE ** (-jnp.arange(half, dtype=F32) * 2.0 / HD)
    angles = positions.astype(F32)[:, None] * inv_freq[None, :]
    cos, sin = jnp.cos(angles), jnp.sin(angles)
    cosine = jnp.concatenate([cos, cos], 1)
    sine = jnp.concatenate([-sin, sin], 1)
    bias = jnp.concatenate((b_query, b_key, b_value))[None, :]
    pos = jnp.pad(positions.astype(F32).reshape(rows // 128, 128), ((0, 8 - rows // 128), (0, 0)))
    any_, vmem = pl.BlockSpec(memory_space=pl.ANY), pl.BlockSpec(memory_space=pltpu.VMEM)
    dma = pltpu.SemaphoreType.DMA
    return pl.pallas_call(
        block_kernel,
        name="block",
        out_shape=(
            jax.ShapeDtypeStruct((rows, feats), BF16),
            jax.ShapeDtypeStruct((rows, qc), BF16),
        ),
        in_specs=[any_, any_, vmem, any_, any_, any_, vmem, vmem, vmem, any_],
        out_specs=(any_, any_),
        scratch_shapes=[
            pltpu.VMEM((nt, rows, feats), BF16),
            pltpu.VMEM((ns, wrows, qc + 2 * kc), BF16),
            pltpu.VMEM((rows, qc + 2 * kc), F32),
            pltpu.VMEM((rows, feats), BF16),
            pltpu.VMEM((nt, 8, 128), F32),
            pltpu.VMEM((rows, 128), F32),
            pltpu.VMEM((nt, w_out.shape[0] // 8, w_out.shape[1]), BF16),
            pltpu.VMEM((ns, 8, 128), F32),
            pltpu.VMEM((heads, rows, HD), BF16),
            pltpu.VMEM((ns * rows, 2 * HD), BF16),
            pltpu.VMEM((nt, 8, qc // 8, feats), BF16),
            pltpu.VMEM((rows, nt * qc), BF16),
            pltpu.VMEM((ns, 1, rows), F32),
            pltpu.VMEM((rows, 128), F32),
            pltpu.VMEM((heads, rows, 128), F32),
            pltpu.VMEM((heads, rows, 128), F32),
            pltpu.VMEM((heads, rows, HD), F32),
            pltpu.VMEM((rows, feats), BF16),
            dma((10,)), dma((20,)), dma((20,)), dma((20,)), dma((20,)),
            dma((8,)), dma((8,)), dma((16,)), dma((16,)), dma((16,)), dma((16,)),
            dma((20,)), dma((20,)), dma((20,)), dma((20,)), dma((48,)), dma((48,)),
        ],
        compiler_params=pltpu.CompilerParams(
            collective_id=0, has_side_effects=True, vmem_limit_bytes=62 * 1024 * 1024
        ),
    )(tokens, pos, norm_gain.reshape(nt, 1, feats), w_query, w_key, w_value, bias, cosine, sine, w_out)


def solution(mesh):
    in_specs = (
        P("seq", "tensor"),
        P("seq"),
        P(),
        P("seq", "tensor"),
        P("seq", "tensor"),
        P("seq", "tensor"),
        P("tensor"),
        P("tensor"),
        P("tensor"),
        P("tensor", "seq"),
    )
    out_specs = (P("seq", "tensor"), P("seq", "tensor"))
    return jax.shard_map(shards, mesh=mesh, in_specs=in_specs, out_specs=out_specs, check_vma=False)
```

```python
import functools
import math

import jax
import jax.numpy as jnp
from jax import lax
from jax.experimental import pallas as pl
from jax.experimental.pallas import tpu as pltpu
from jax.sharding import PartitionSpec as P

HD = 128
NORM_EPS = 1e-06
ROPE_BASE = 1000000.0
NEG_FILL = -1e30
MESH = pl.DeviceIdType.MESH
BF16 = jnp.bfloat16
F32 = jnp.float32


def coords():
    s, t = lax.axis_index("seq"), lax.axis_index("tensor")
    return dict(y=s // 4, zl=(s // 2) % 2, c=s % 2, zh=t // 4, x=t % 4)


SIZES = dict(y=4, zl=2, c=2, zh=2, x=4)


def moved(k, **shift):
    k = dict(k)
    for name, by in shift.items():
        k[name] = (k[name] + (by + SIZES[name])) % SIZES[name]
    return k


def seq_of(k):
    return k["y"] * 4 + k["zl"] * 2 + k["c"]


def tensor_of(k):
    return k["zh"] * 4 + k["x"]


def device(k):
    return (seq_of(k), tensor_of(k))


class Gather:
    def __init__(self, k, slot, half_rows, ring, pair, sibling, ssem, rsem, base=0, along=0):
        self.k, self.slot, self.half = k, slot, half_rows
        self.ring, self.pair, self.sibling = ring, pair, sibling
        self.ssem, self.rsem, self.base = ssem, rsem, base
        self.along, self.direct = along, 2 * half_rows - 2 * along
        self.sent = []

    def at(self, r=0, p=0, c=0):
        return (r, p, c)

    def place(self, where):
        r, p, c = where
        return moved(self.k, **{self.ring: r, self.pair: p, "c": c})

    def copy(self, i, block, target, half):
        ref = self.slot(self.place(block))
        if half is not None:
            first, count = half if isinstance(half, tuple) else (half * self.half, self.half)
            ref = ref.at[pl.ds(first, count)]
        return pltpu.make_async_remote_copy(
            src_ref=ref,
            dst_ref=ref,
            send_sem=self.ssem.at[self.base + i],
            recv_sem=self.rsem.at[self.base + i],
            device_id=device(self.place(target)),
            device_id_type=MESH,
        )

    def send(self, i, block, target, half=None):
        self.copy(i, block, target, half).start()
        self.sent.append((i, block, target, half))

    def recv(self, i, block, half=None):
        self.copy(i, block, (0, 0, 1) if self.sibling else (1, 0, 0), half).wait_recv()

    def share(self, i, block):
        if self.sibling:
            self.send(i, block, self.at(c=1))

    def s0(self):
        own = self.at()
        self.send(0, own, self.at(1))
        self.send(1, own, self.at(-1))
        if self.sibling:
            self.send(2, own, self.at(p=1))
        self.share(3, own)

    def s0_ring(self):
        self.send(0, self.at(), self.at(1))
        self.send(1, self.at(), self.at(-1))
        self.share(3, self.at())

    def s0_pair(self):
        self.send(2, self.at(), self.at(p=1))

    def pair_halves(self):
        self.send(2, self.at(), self.at(p=1), 0)
        self.send(3, self.at(), self.at(p=1), 1)

    def s1(self):
        self.recv(0, self.at(-1))
        self.send(4, self.at(-1), self.at(1), 0)
        self.share(5, self.at(-1))
        self.recv(1, self.at(1))
        self.send(6, self.at(1), self.at(-1), 1)
        self.share(7, self.at(1))

    def s2(self):
        self.recv(2, self.at(p=1))
        self.send(8, self.at(p=1), self.at(1))
        self.send(9, self.at(p=1), self.at(-1))
        self.share(10, self.at(p=1))

    def s2_half(self, h):
        self.recv(2 + h, self.at(p=1), h)
        self.send(8 + 2 * h, self.at(p=1), self.at(1), h)
        self.send(9 + 2 * h, self.at(p=1), self.at(-1), h)

    def s4_halves(self):
        for h in (0, 1):
            self.recv(8 + 2 * h, self.at(-1, 1), h)
            self.recv(9 + 2 * h, self.at(1, 1), h)
        if self.along:
            self.send(14, self.at(-1, 1), self.at(1), (self.direct, self.along))
            self.send(15, self.at(1, 1), self.at(-1), (self.direct + self.along, self.along))

    def s3(self):
        self.recv(4, self.at(2), 0)
        self.recv(6, self.at(2), 1)
        self.share(11, self.at(2))
        if not self.sibling:
            self.send(13, self.at(2), self.at(p=1), (0, self.direct))

    def s4(self):
        self.recv(8, self.at(-1, 1))
        if self.sibling:
            self.send(13, self.at(-1, 1), self.at(1), 0)
        self.share(14, self.at(-1, 1))
        self.recv(9, self.at(1, 1))
        if self.sibling:
            self.send(15, self.at(1, 1), self.at(-1), 1)
        self.share(16, self.at(1, 1))

    def s5(self):
        if self.sibling:
            self.recv(13, self.at(2, 1), 0)
            self.recv(15, self.at(2, 1), 1)
            self.share(17, self.at(2, 1))
        else:
            self.recv(13, self.at(2, 1), (0, self.direct))
            if self.along:
                self.recv(14, self.at(2, 1), (self.direct, self.along))
                self.recv(15, self.at(2, 1), (self.direct + self.along, self.along))

    SHARED = {(0, 0): 3, (-1, 0): 5, (1, 0): 7, (0, 1): 10, (2, 0): 11, (-1, 1): 14, (1, 1): 16, (2, 1): 17}

    def recv_sibling(self, r, p):
        self.recv(self.SHARED[(r, p)], self.at(r, p, 1))

    def finish(self):
        for i, block, target, half in self.sent:
            self.copy(i, block, target, half).wait_send()


ORDER = ((0, 0), (-1, 0), (1, 0), (0, 1), (2, 0), (-1, 1), (1, 1), (2, 1))


def pick(index, values):
    out = values[0]
    for i, v in enumerate(values[1:], 1):
        out = jnp.where(index == i, v, out)
    return out


def greet(k, peers):
    barrier = pltpu.get_barrier_semaphore()
    for p in peers:
        pl.semaphore_signal(barrier, inc=1, device_id=device(p), device_id_type=MESH)
    pl.semaphore_wait(barrier, len(peers))


def tensor_peers(k):
    return [moved(k, x=r, zh=p) for r, p in ORDER[1:]]


def seq_peers(k):
    return [
        moved(k, y=r, zl=p, c=c) for r, p in ORDER for c in (0, 1) if (r, p, c) != (0, 0, 0)
    ]


def as_columns(rows):
    parts = [jnp.broadcast_to(rows[i : i + 1, :], (128, 128)).T for i in range(rows.shape[0])]
    return jnp.concatenate(parts, 0)


QT = 128
CHUNKS = ((0, 2), (2, 1), (3, 1))
GROUP = 2
ALONG = 64


def block_kernel(
    tokens, pos, gain, w_query, w_key, w_value, bias, cosine, sine, w_out,
    mixed, context,
    x_all, w_all, acc, normed, ssq, inverse, wo_mid, pos_all,
    q, kv_all, wo_all, ctx_all, key_pos, own_pos, top, low, num,
    local_sem, x_ssem, x_rsem, w_ssem, w_rsem, s_ssem, s_rsem, p_ssem, p_rsem, t_ssem, t_rsem,
    kv_ssem, kv_rsem, wo_ssem, wo_rsem, c_ssem, c_rsem,
):
    k = coords()
    me_s, me_t = seq_of(k), tensor_of(k)
    rows = tokens.shape[0]
    qc, kc = w_query.shape[1], w_key.shape[1]
    wrows = w_query.shape[0]
    heads = qc // HD
    cw = qc

    loads = [
        pltpu.make_async_copy(tokens, x_all.at[me_t], local_sem.at[0]),
        pltpu.make_async_copy(w_query, w_all.at[me_s, :, pl.ds(0, qc)], local_sem.at[1]),
        pltpu.make_async_copy(w_key, w_all.at[me_s, :, pl.ds(qc, kc)], local_sem.at[2]),
        pltpu.make_async_copy(w_value, w_all.at[me_s, :, pl.ds(qc + kc, kc)], local_sem.at[3]),
        pltpu.make_async_copy(pos, pos_all.at[me_s], local_sem.at[4]),
    ]
    for c in loads:
        c.start()
    greet(k, tensor_peers(k) + seq_peers(k))
    for c in loads:
        c.wait()

    def wo_slot(b):
        return wo_all.at[:, seq_of(b) // 2, :, pl.ds(pl.multiple_of(b["c"] * cw, cw), cw)]

    def ctx_slot(first, count):
        return lambda b: ctx_all.at[
            pl.ds(first * QT, count * QT), pl.ds(pl.multiple_of(tensor_of(b) * cw, cw), cw)
        ]

    xg = Gather(k, lambda b: x_all.at[tensor_of(b)], rows // 2, "x", "zh", False, x_ssem, x_rsem, along=ALONG)
    wg = Gather(k, lambda b: w_all.at[seq_of(b)], wrows // 2, "y", "zl", True, w_ssem, w_rsem)
    kg = Gather(
        k, lambda b: kv_all.at[pl.ds(pl.multiple_of(seq_of(b) * rows, rows), rows)], rows // 2,
        "y", "zl", True, kv_ssem, kv_rsem,
    )
    og = Gather(k, wo_slot, wo_all.shape[0] // 2, "y", "zl", True, wo_ssem, wo_rsem)
    cg = [
        Gather(k, ctx_slot(f, n), n * QT // 2, "x", "zh", False, c_ssem, c_rsem, base=16 * i)
        for i, (f, n) in enumerate(CHUNKS)
    ]

    eighth = wo_mid.shape[1]

    def spread_copy(i, source, target):
        return pltpu.make_async_remote_copy(
            w_out.at[pl.ds((seq_of(target) // 2) * eighth, eighth)], wo_mid.at[seq_of(source) // 2],
            t_ssem.at[i], t_rsem.at[i], device_id=device(target), device_id_type=MESH,
        )

    def wo_part(t):
        return wo_all.at[t, me_s // 2, :, pl.ds(pl.multiple_of(k["c"] * cw, cw), cw)]

    def settle_copy(i, source, target):
        return pltpu.make_async_remote_copy(
            wo_mid.at[tensor_of(target)], wo_part(tensor_of(source)),
            t_ssem.at[8 + i], t_rsem.at[8 + i], device_id=device(target), device_id_type=MESH,
        )

    spread_own = pltpu.make_async_copy(
        w_out.at[pl.ds((me_s // 2) * eighth, eighth)], wo_mid.at[me_s // 2], t_ssem.at[7]
    )
    settle_own = pltpu.make_async_copy(wo_mid.at[me_t], wo_part(me_t), t_ssem.at[15])

    def pos_copy(i, b, target):
        ref = pos_all.at[seq_of(b)]
        return pltpu.make_async_remote_copy(
            ref, ref, p_ssem.at[i], p_rsem.at[i], device_id=device(target), device_id_type=MESH
        )

    s_list = [(r, p, c) for r, p in ORDER for c in (0, 1) if (r, p, c) != (0, 0, 0)]

    def ssq_copy(i, b, target):
        ref = ssq.at[tensor_of(b)]
        return pltpu.make_async_remote_copy(
            ref, ref, s_ssem.at[i], s_rsem.at[i], device_id=device(target), device_id_type=MESH
        )

    wg.s0()
    xg.s0()
    for i in range(rows // 128):
        xb = x_all[me_t, pl.ds(i * 128, 128), :].astype(F32)
        total = jnp.sum(xb * xb, -1, keepdims=True)
        ssq[me_t, i : i + 1, :] = jnp.broadcast_to(total, (128, 128)).T[0:1, :]
    for i, (r, p) in enumerate(ORDER[1:]):
        spread_copy(i, k, moved(k, y=r, zl=p)).start()
    spread_own.start()
    for i, (r, p, c) in enumerate(s_list):
        pos_copy(i, k, moved(k, y=r, zl=p, c=c)).start()
    acc[...] = jnp.zeros_like(acc)
    top[...] = jnp.full_like(top, NEG_FILL)
    low[...] = jnp.zeros_like(low)
    num[...] = jnp.zeros_like(num)
    for i, (r, p) in enumerate(ORDER[1:]):
        ssq_copy(i, k, moved(k, x=r, zh=p)).start()

    wg.s1()
    wg.s2()
    xg.pair_halves()
    xg.s1()
    for i, (r, p) in enumerate(ORDER[1:]):
        ssq_copy(i, moved(k, x=-r, zh=p), k).wait_recv()
    total = ssq[0]
    for i in range(1, 8):
        total = total + ssq[i]
    scale = lax.rsqrt(total / (8 * x_all.shape[2]) + NORM_EPS)
    inverse[...] = as_columns(scale[0 : rows // 128, :])
    wg.s3()
    xg.s2_half(0)
    for i, (r, p) in enumerate(ORDER[1:]):
        spread_copy(i, moved(k, y=-r, zl=p), moved(k, y=r, zl=p)).wait_recv()
    spread_own.wait()
    for i, (r, p) in enumerate(ORDER[1:]):
        settle_copy(i, k, moved(k, x=r, zh=p)).start()
    settle_own.start()
    xg.s3()
    xg.s2_half(1)
    wg.s4()
    for i, (r, p, c) in enumerate(s_list):
        pos_copy(i, moved(k, y=-r, zl=p, c=c), k).wait_recv()

    def spread(s, carry):
        for j in range(rows // 128):
            key_pos[s, :, j * 128 : (j + 1) * 128] = pos_all[s, j : j + 1, :]
        return carry

    lax.fori_loop(0, pos_all.shape[0], spread, 0)
    own_pos[...] = as_columns(pos_all[me_s][0 : rows // 128, :])
    for i, (r, p) in enumerate(ORDER[1:]):
        settle_copy(i, moved(k, x=-r, zh=p), moved(k, x=r, zh=p)).wait_recv()
    settle_own.wait()
    og.s0_ring()
    wg.s5()
    for r, p in ORDER:
        wg.recv_sibling(r, p)

    def block(step, carry):
        @pl.when(step == 5)
        def _():
            xg.s4_halves()

        @pl.when(step == 7)
        def _():
            xg.s5()

        dx = pick(step, [r % 4 for r, _ in ORDER])
        dz = pick(step, [p for _, p in ORDER])
        t = ((k["zh"] + dz) % 2) * 4 + (k["x"] + dx) % 4
        g = gain[t]
        for i in range(rows // 128):
            inv = inverse[pl.ds(i * 128, 128), :]
            for j in range(x_all.shape[2] // 128):
                piece = x_all[t, pl.ds(i * 128, 128), pl.ds(j * 128, 128)].astype(F32)
                normed[pl.ds(i * 128, 128), pl.ds(j * 128, 128)] = (
                    piece * inv * g[:, j * 128 : (j + 1) * 128]
                ).astype(BF16)
        part = jnp.dot(normed[:, 0:wrows], w_all[2 * t], preferred_element_type=F32)
        part = part + jnp.dot(
            normed[:, wrows : 2 * wrows], w_all[2 * t + 1], preferred_element_type=F32
        )
        acc[...] += part
        return carry

    lax.fori_loop(0, 8, block, 0)

    cos, sin = cosine[...], sine[...]
    mine_r = pl.ds(pl.multiple_of(me_s * rows, rows), rows)

    def turned(h):
        u = acc[:, h * HD : (h + 1) * HD] + bias[:, h * HD : (h + 1) * HD]
        return (u * cos + pltpu.roll(u, HD // 2, 1) * sin).astype(BF16)

    kv_all[mine_r, 0:HD] = turned(heads)
    kv_all[mine_r, HD : 2 * HD] = (acc[:, qc + kc :] + bias[:, qc + kc :]).astype(BF16)
    for h in range(heads):
        q[h] = turned(h)
    kg.s0()
    og.s0_pair()

    factor = HD ** (-0.5) / math.log(2.0)
    keys = 2 * rows
    tiles = rows // QT
    events = {}

    def event(step, *fns):
        events.setdefault(step, []).extend(fns)

    def sib(r, p):
        return lambda: kg.recv_sibling(r, p)

    def close(i):
        f, n = CHUNKS[i]
        r = pl.ds(f * QT, n * QT)
        for h in range(heads):
            bottom = jnp.sum(low[h, r, :], -1, keepdims=True)
            done = (num[h, r, :] / bottom).astype(BF16)
            ctx_all[r, pl.ds(pl.multiple_of(me_t * cw + h * HD, HD), HD)] = done
            context[r, h * HD : (h + 1) * HD] = done

    def send_ctx(i):
        cg[i].s0()
        cg[i].pair_halves()

    def settle_sends():
        for i, (r, p) in enumerate(ORDER[1:]):
            spread_copy(i, k, moved(k, y=r, zl=p)).wait_send()
            settle_copy(i, k, moved(k, x=r, zh=p)).wait_send()
            ssq_copy(i, k, moved(k, x=r, zh=p)).wait_send()
        for i, (r, p, c) in enumerate(s_list):
            pos_copy(i, k, moved(k, y=r, zl=p, c=c)).wait_send()
        xg.finish()
        wg.finish()

    event(0, sib(0, 0))
    event(2, kg.s1, sib(-1, 0))
    event(3, kg.s2, settle_sends, sib(1, 0))
    event(4, sib(0, 1))
    event(5, kg.s3, sib(2, 0))
    event(6, kg.s4, sib(-1, 1), og.s1)
    event(7, sib(1, 1))
    event(8, kg.s5, sib(2, 1), og.s2)
    event(9, lambda: close(0), lambda: send_ctx(0))
    event(12, cg[0].s1)
    event(13, lambda: close(1), lambda: send_ctx(1), lambda: cg[0].s2_half(0), lambda: cg[0].s2_half(1))
    event(14, cg[0].s3, og.s3)

    def step(g, carry):
        for at, fns in sorted(events.items()):
            @pl.when(g == at)
            def _(fns=fns):
                for fn in fns:
                    fn()

        units = [Unit(2 * g + half, u) for half in range(2) for u in range(heads // GROUP)]
        s, held = units[0].scores(), None
        for i, unit in enumerate(units):
            later = units[i + 1].scores() if i + 1 < len(units) else None
            now = unit.soften(s)
            if held is not None:
                units[i - 1].collect(*held)
            s, held = later, now
        units[-1].collect(*held)
        return carry

    class Unit:
        def __init__(self, g, u):
            late = jnp.maximum(g - 18, 0)
            mid = jnp.maximum(g - 4, 0)
            kb = jnp.where(g < 4, 0, jnp.where(g < 18, 1 + mid // 2, 1 + late % 7))
            tile = jnp.where(g < 4, g, jnp.where(g < 18, mid % 2, 2 + late // 7))
            dy = pick(kb, [r % 4 for r, _ in ORDER])
            dz = pick(kb, [p for _, p in ORDER])
            self.chip = ((k["y"] + dy) % 4) * 2 + (k["zl"] + dz) % 2
            self.kr = pl.ds(pl.multiple_of(self.chip * keys, keys), keys)
            self.at = (slice(u * GROUP, (u + 1) * GROUP), pl.ds(pl.multiple_of(tile * QT, QT), QT), slice(None))
            self.mine = jnp.concatenate([own_pos[self.at[1], :]] * GROUP, 0)

        def scores(self):
            return lax.dot_general(
                q[self.at].reshape(GROUP * QT, HD), kv_all[self.kr, 0:HD], (((1,), (1,)), ((), ())),
                preferred_element_type=F32,
            )

        def soften(self, s):
            parts = []
            for j in range(keys // 128):
                lane = (j % (rows // 128)) * 128
                kp = key_pos[self.chip * 2 + j // (rows // 128), :, lane : lane + 128]
                parts.append(jnp.where(kp <= self.mine, s[:, j * 128 : (j + 1) * 128], NEG_FILL))
            best = parts[0]
            for x in parts[1:]:
                best = jnp.maximum(best, x)
            old = top[self.at].reshape(GROUP * QT, 128)
            new = jnp.maximum(old, jnp.max(best, -1, keepdims=True))
            top[self.at] = new.reshape(GROUP, QT, 128)
            alpha = jnp.exp2((old - new) * factor)
            weights, total = [], low[self.at].reshape(GROUP * QT, 128) * alpha
            for x in parts:
                w = jnp.exp2((x - new) * factor)
                total = total + w
                weights.append(w.astype(BF16))
            low[self.at] = total.reshape(GROUP, QT, 128)
            return alpha, jnp.concatenate(weights, 1)

        def collect(self, alpha, weights):
            out = num[self.at].reshape(GROUP * QT, HD) * alpha + jnp.dot(
                weights, kv_all[self.kr, HD : 2 * HD], preferred_element_type=F32
            )
            num[self.at] = out.reshape(GROUP, QT, HD)

    lax.fori_loop(0, 4 * tiles, step, 0)

    close(2)
    send_ctx(2)
    def output(first, count):
        r = pl.ds(first * QT, count * QT)

        def part(c, carry):
            cols = pl.ds(pl.multiple_of(c * 256, 256), 256)
            w = wo_all[:, :, :, cols].reshape(ctx_all.shape[1], 256)
            summed = jnp.dot(ctx_all[r, :], w, preferred_element_type=F32)
            mixed[r, cols] = (x_all[me_t, r, cols].astype(F32) + summed).astype(BF16)
            return carry

        lax.fori_loop(0, mixed.shape[1] // 256, part, 0)

    cg[1].s1()
    cg[1].s2_half(0)
    cg[1].s2_half(1)
    og.s4()
    og.s5()
    for r, p in ORDER:
        og.recv_sibling(r, p)
    cg[0].s4_halves()
    cg[0].s5()
    cg[1].s3()
    cg[2].s1()
    cg[2].s2_half(0)
    cg[2].s2_half(1)
    output(0, 2)
    cg[2].s3()
    cg[1].s4_halves()
    cg[1].s5()
    output(2, 1)
    kg.finish()
    og.finish()
    cg[2].s4_halves()
    cg[2].s5()
    output(3, 1)
    for x in cg:
        x.finish()


def shards(tokens, positions, norm_gain, w_query, w_key, w_value, b_query, b_key, b_value, w_out):
    rows, feats = tokens.shape
    qc, kc = w_query.shape[1], w_key.shape[1]
    wrows = w_query.shape[0]
    heads = qc // HD
    nt, ns = lax.axis_size("tensor"), lax.axis_size("seq")
    half = HD // 2
    inv_freq = ROPE_BASE ** (-jnp.arange(half, dtype=F32) * 2.0 / HD)
    angles = positions.astype(F32)[:, None] * inv_freq[None, :]
    cos, sin = jnp.cos(angles), jnp.sin(angles)
    cosine = jnp.concatenate([cos, cos], 1)
    sine = jnp.concatenate([-sin, sin], 1)
    bias = jnp.concatenate((b_query, b_key, b_value))[None, :]
    pos = jnp.pad(positions.astype(F32).reshape(rows // 128, 128), ((0, 8 - rows // 128), (0, 0)))
    any_, vmem = pl.BlockSpec(memory_space=pltpu.HBM), pl.BlockSpec(memory_space=pltpu.VMEM)
    dma = pltpu.SemaphoreType.DMA
    return pl.pallas_call(
        block_kernel,
        name="block",
        out_shape=(
            jax.ShapeDtypeStruct((rows, feats), BF16),
            jax.ShapeDtypeStruct((rows, qc), BF16),
        ),
        in_specs=[any_, any_, vmem, any_, any_, any_, vmem, vmem, vmem, any_],
        out_specs=(vmem, vmem),
        scratch_shapes=[
            pltpu.VMEM((nt, rows, feats), BF16),
            pltpu.VMEM((ns, wrows, qc + 2 * kc), BF16),
            pltpu.VMEM((rows, qc + 2 * kc), F32),
            pltpu.VMEM((rows, feats), BF16),
            pltpu.VMEM((nt, 8, 128), F32),
            pltpu.VMEM((rows, 128), F32),
            pltpu.VMEM((nt, w_out.shape[0] // 8, w_out.shape[1]), BF16),
            pltpu.VMEM((ns, 8, 128), F32),
            pltpu.VMEM((heads, rows, HD), BF16),
            pltpu.VMEM((ns * rows, 2 * HD), BF16),
            pltpu.VMEM((nt, 8, qc // 8, feats), BF16),
            pltpu.VMEM((rows, nt * qc), BF16),
            pltpu.VMEM((ns, 1, rows), F32),
            pltpu.VMEM((rows, 128), F32),
            pltpu.VMEM((heads, rows, 128), F32),
            pltpu.VMEM((heads, rows, 128), F32),
            pltpu.VMEM((heads, rows, HD), F32),
            dma((10,)), dma((20,)), dma((20,)), dma((20,)), dma((20,)),
            dma((8,)), dma((8,)), dma((16,)), dma((16,)), dma((16,)), dma((16,)),
            dma((20,)), dma((20,)), dma((20,)), dma((20,)), dma((48,)), dma((48,)),
        ],
        compiler_params=pltpu.CompilerParams(
            collective_id=0, has_side_effects=True, vmem_limit_bytes=56 * 1024 * 1024
        ),
    )(tokens, pos, norm_gain.reshape(nt, 1, feats), w_query, w_key, w_value, bias, cosine, sine, w_out)


def solution(mesh):
    in_specs = (
        P("seq", "tensor"),
        P("seq"),
        P(),
        P("seq", "tensor"),
        P("seq", "tensor"),
        P("seq", "tensor"),
        P("tensor"),
        P("tensor"),
        P("tensor"),
        P("tensor", "seq"),
    )
    out_specs = (P("seq", "tensor"), P("seq", "tensor"))
    return jax.shard_map(shards, mesh=mesh, in_specs=in_specs, out_specs=out_specs, check_vma=False)
```

```python
import functools
import math

import jax
import jax.numpy as jnp
from jax import lax
from jax.experimental import pallas as pl
from jax.experimental.pallas import tpu as pltpu
from jax.sharding import PartitionSpec as P

HD = 128
NORM_EPS = 1e-06
ROPE_BASE = 1000000.0
NEG_FILL = -1e30
MESH = pl.DeviceIdType.MESH
BF16 = jnp.bfloat16
F32 = jnp.float32


def coords():
    s, t = lax.axis_index("seq"), lax.axis_index("tensor")
    return dict(y=s // 4, zl=(s // 2) % 2, c=s % 2, zh=t // 4, x=t % 4)


SIZES = dict(y=4, zl=2, c=2, zh=2, x=4)


def moved(k, **shift):
    k = dict(k)
    for name, by in shift.items():
        k[name] = (k[name] + (by + SIZES[name])) % SIZES[name]
    return k


def seq_of(k):
    return k["y"] * 4 + k["zl"] * 2 + k["c"]


def tensor_of(k):
    return k["zh"] * 4 + k["x"]


def device(k):
    return (seq_of(k), tensor_of(k))


class Gather:
    def __init__(self, k, slot, half_rows, ring, pair, sibling, ssem, rsem, base=0, along=0, far_by_pair=False):
        self.k, self.slot, self.half = k, slot, half_rows
        self.ring, self.pair, self.sibling = ring, pair, sibling
        self.ssem, self.rsem, self.base = ssem, rsem, base
        self.along, self.direct = along, 2 * half_rows - 2 * along
        self.far_by_pair = far_by_pair or not sibling
        self.sent = []

    def at(self, r=0, p=0, c=0):
        return (r, p, c)

    def place(self, where):
        r, p, c = where
        return moved(self.k, **{self.ring: r, self.pair: p, "c": c})

    def copy(self, i, block, target, half):
        ref = self.slot(self.place(block))
        if half is not None:
            first, count = half if isinstance(half, tuple) else (half * self.half, self.half)
            ref = ref.at[pl.ds(first, count)]
        return pltpu.make_async_remote_copy(
            src_ref=ref,
            dst_ref=ref,
            send_sem=self.ssem.at[self.base + i],
            recv_sem=self.rsem.at[self.base + i],
            device_id=device(self.place(target)),
            device_id_type=MESH,
        )

    def send(self, i, block, target, half=None):
        self.copy(i, block, target, half).start()
        self.sent.append((i, block, target, half))

    def recv(self, i, block, half=None):
        self.copy(i, block, (0, 0, 1) if self.sibling else (1, 0, 0), half).wait_recv()

    def share(self, i, block):
        if self.sibling:
            self.send(i, block, self.at(c=1))

    def s0(self):
        self.s0_ring()
        self.s0_pair()

    def s0_ring(self):
        self.send(0, self.at(), self.at(1))
        self.send(1, self.at(), self.at(-1))
        self.share(3, self.at())

    def s0_pair(self):
        self.send(2, self.at(), self.at(p=1))

    def s1(self):
        self.recv(0, self.at(-1))
        self.send(4, self.at(-1), self.at(1), 0)
        self.share(5, self.at(-1))
        self.recv(1, self.at(1))
        self.send(6, self.at(1), self.at(-1), 1)
        self.share(7, self.at(1))

    def s2(self):
        self.recv(2, self.at(p=1))
        self.send(8, self.at(p=1), self.at(1))
        self.send(9, self.at(p=1), self.at(-1))
        self.share(10, self.at(p=1))

    def s3(self):
        self.recv(4, self.at(2), 0)
        self.recv(6, self.at(2), 1)
        self.share(11, self.at(2))
        if self.far_by_pair:
            self.send(13, self.at(2), self.at(p=1), (0, self.direct))

    def s4(self):
        self.recv(8, self.at(-1, 1))
        if not self.far_by_pair:
            self.send(13, self.at(-1, 1), self.at(1), 0)
        elif self.along:
            self.send(14, self.at(-1, 1), self.at(1), (self.direct, self.along))
        self.share(14, self.at(-1, 1))
        self.recv(9, self.at(1, 1))
        if not self.far_by_pair:
            self.send(15, self.at(1, 1), self.at(-1), 1)
        elif self.along:
            self.send(15, self.at(1, 1), self.at(-1), (self.direct + self.along, self.along))
        self.share(16, self.at(1, 1))

    def s5(self):
        if self.far_by_pair:
            self.recv(13, self.at(2, 1), (0, self.direct))
            if self.along:
                self.recv(14, self.at(2, 1), (self.direct, self.along))
                self.recv(15, self.at(2, 1), (self.direct + self.along, self.along))
        else:
            self.recv(13, self.at(2, 1), 0)
            self.recv(15, self.at(2, 1), 1)
        self.share(17, self.at(2, 1))

    SHARED = {(0, 0): 3, (-1, 0): 5, (1, 0): 7, (0, 1): 10, (2, 0): 11, (-1, 1): 14, (1, 1): 16, (2, 1): 17}

    def recv_sibling(self, r, p):
        self.recv(self.SHARED[(r, p)], self.at(r, p, 1))

    def finish(self):
        for i, block, target, half in self.sent:
            self.copy(i, block, target, half).wait_send()


ORDER = ((0, 0), (-1, 0), (1, 0), (0, 1), (2, 0), (-1, 1), (1, 1), (2, 1))


def pick(index, values):
    out = values[0]
    for i, v in enumerate(values[1:], 1):
        out = jnp.where(index == i, v, out)
    return out


def greet(k, peers):
    barrier = pltpu.get_barrier_semaphore()
    for p in peers:
        pl.semaphore_signal(barrier, inc=1, device_id=device(p), device_id_type=MESH)
    pl.semaphore_wait(barrier, len(peers))


def tensor_peers(k):
    return [moved(k, x=r, zh=p) for r, p in ORDER[1:]]


def seq_peers(k):
    return [
        moved(k, y=r, zl=p, c=c) for r, p in ORDER for c in (0, 1) if (r, p, c) != (0, 0, 0)
    ]


def as_columns(rows):
    parts = [jnp.broadcast_to(rows[i : i + 1, :], (128, 128)).T for i in range(rows.shape[0])]
    return jnp.concatenate(parts, 0)


QT = 128
CHUNKS = ((0, 2), (2, 1), (3, 1))
GROUP = 2
ALONG = (64, 0)


def block_kernel(
    tokens, pos, gain, w_query, w_key, w_value, bias, cosine, sine, w_out,
    mixed, context,
    x_all, w_all, acc, normed, ssq, inverse, wo_mid, pos_all,
    q, kv_all, wo_all, ctx_all, key_pos, own_pos, top, low, num, mixed_v,
    local_sem, x_ssem, x_rsem, w_ssem, w_rsem, s_ssem, s_rsem, p_ssem, p_rsem, t_ssem, t_rsem,
    kv_ssem, kv_rsem, wo_ssem, wo_rsem, c_ssem, c_rsem,
):
    k = coords()
    me_s, me_t = seq_of(k), tensor_of(k)
    rows = tokens.shape[0]
    qc, kc = w_query.shape[1], w_key.shape[1]
    wrows = w_query.shape[0]
    heads = qc // HD
    cw = qc

    loads = [
        pltpu.make_async_copy(tokens, x_all.at[me_t], local_sem.at[0]),
        pltpu.make_async_copy(w_query, w_all.at[me_s, :, pl.ds(0, qc)], local_sem.at[1]),
        pltpu.make_async_copy(w_key, w_all.at[me_s, :, pl.ds(qc, kc)], local_sem.at[2]),
        pltpu.make_async_copy(w_value, w_all.at[me_s, :, pl.ds(qc + kc, kc)], local_sem.at[3]),
        pltpu.make_async_copy(pos, pos_all.at[me_s], local_sem.at[4]),
    ]
    for c in loads:
        c.start()
    greet(k, tensor_peers(k) + seq_peers(k))
    for c in loads:
        c.wait()

    def wo_slot(b):
        return wo_all.at[:, seq_of(b) // 2, :, pl.ds(pl.multiple_of(b["c"] * cw, cw), cw)]

    def ctx_slot(first, count):
        return lambda b: ctx_all.at[
            pl.ds(first * QT, count * QT), pl.ds(pl.multiple_of(tensor_of(b) * cw, cw), cw)
        ]

    part_rows = rows // 2
    xg = [
        Gather(
            k, lambda b, h=h: x_all.at[tensor_of(b), pl.ds(h * part_rows, part_rows)], part_rows // 2,
            "x", "zh", False, x_ssem, x_rsem, base=20 * h, along=ALONG[h],
        )
        for h in range(2)
    ]
    wg = Gather(k, lambda b: w_all.at[seq_of(b)], wrows // 2, "y", "zl", True, w_ssem, w_rsem)
    def kv_rows(h, b):
        return pl.ds(pl.multiple_of((h * 16 + seq_of(b)) * part_rows, part_rows), part_rows)

    kg = [
        Gather(
            k, lambda b, h=h: kv_all.at[kv_rows(h, b)], part_rows // 2, "y", "zl", True,
            kv_ssem, kv_rsem, base=20 * h, far_by_pair=h == 1,
        )
        for h in range(2)
    ]
    og = Gather(
        k, wo_slot, wo_all.shape[0] // 2, "y", "zl", True, wo_ssem, wo_rsem
    )
    cg = [
        Gather(k, ctx_slot(f, n), n * QT // 2, "x", "zh", False, c_ssem, c_rsem, base=16 * i)
        for i, (f, n) in enumerate(CHUNKS)
    ]

    eighth = wo_mid.shape[1]

    def spread_copy(i, source, target):
        return pltpu.make_async_remote_copy(
            w_out.at[pl.ds((seq_of(target) // 2) * eighth, eighth)], wo_mid.at[seq_of(source) // 2],
            t_ssem.at[i], t_rsem.at[i], device_id=device(target), device_id_type=MESH,
        )

    def wo_part(t):
        return wo_all.at[t, me_s // 2, :, pl.ds(pl.multiple_of(k["c"] * cw, cw), cw)]

    def settle_copy(i, source, target):
        return pltpu.make_async_remote_copy(
            wo_mid.at[tensor_of(target)], wo_part(tensor_of(source)),
            t_ssem.at[8 + i], t_rsem.at[8 + i], device_id=device(target), device_id_type=MESH,
        )

    spread_own = pltpu.make_async_copy(
        w_out.at[pl.ds((me_s // 2) * eighth, eighth)], wo_mid.at[me_s // 2], t_ssem.at[7]
    )
    settle_own = pltpu.make_async_copy(wo_mid.at[me_t], wo_part(me_t), t_ssem.at[15])

    def pos_copy(i, b, target):
        ref = pos_all.at[seq_of(b)]
        return pltpu.make_async_remote_copy(
            ref, ref, p_ssem.at[i], p_rsem.at[i], device_id=device(target), device_id_type=MESH
        )

    s_list = [(r, p, c) for r, p in ORDER for c in (0, 1) if (r, p, c) != (0, 0, 0)]

    def ssq_copy(i, b, target):
        ref = ssq.at[tensor_of(b)]
        return pltpu.make_async_remote_copy(
            ref, ref, s_ssem.at[i], s_rsem.at[i], device_id=device(target), device_id_type=MESH
        )

    wg.s0()
    xg[0].s0_ring()
    xg[1].s0_ring()
    for i in range(rows // 128):
        xb = x_all[me_t, pl.ds(i * 128, 128), :].astype(F32)
        total = jnp.sum(xb * xb, -1, keepdims=True)
        ssq[me_t, i : i + 1, :] = jnp.broadcast_to(total, (128, 128)).T[0:1, :]
    for i, (r, p, c) in enumerate(s_list):
        pos_copy(i, k, moved(k, y=r, zl=p, c=c)).start()
    acc[...] = jnp.zeros_like(acc)
    top[...] = jnp.full_like(top, NEG_FILL)
    low[...] = jnp.zeros_like(low)
    num[...] = jnp.zeros_like(num)
    for i, (r, p) in enumerate(ORDER[1:]):
        ssq_copy(i, k, moved(k, x=r, zh=p)).start()

    wg.s1()
    wg.s2()
    xg[0].s0_pair()
    xg[0].s1()
    xg[1].s1()
    for i, (r, p) in enumerate(ORDER[1:]):
        ssq_copy(i, moved(k, x=-r, zh=p), k).wait_recv()
    total = ssq[0]
    for i in range(1, 8):
        total = total + ssq[i]
    scale = lax.rsqrt(total / (8 * x_all.shape[2]) + NORM_EPS)
    inverse[...] = as_columns(scale[0 : rows // 128, :])
    wg.s3()
    xg[0].s3()
    xg[1].s0_pair()
    xg[0].s2()
    xg[1].s3()
    wg.s4()
    for i, (r, p) in enumerate(ORDER[1:]):
        spread_copy(i, k, moved(k, y=r, zl=p)).start()
    spread_own.start()
    xg[0].s4()
    xg[1].s2()
    for i, (r, p, c) in enumerate(s_list):
        pos_copy(i, moved(k, y=-r, zl=p, c=c), k).wait_recv()

    def spread(s, carry):
        for h in range(2):
            for j in range(part_rows // 128):
                row = h * (part_rows // 128) + j
                key_pos[h * 16 + s, :, j * 128 : (j + 1) * 128] = pos_all[s, row : row + 1, :]
        return carry

    lax.fori_loop(0, pos_all.shape[0], spread, 0)
    own_pos[...] = as_columns(pos_all[me_s][0 : rows // 128, :])
    def settle():
        for i, (r, p) in enumerate(ORDER[1:]):
            spread_copy(i, moved(k, y=-r, zl=p), moved(k, y=r, zl=p)).wait_recv()
        spread_own.wait()
        for i, (r, p) in enumerate(ORDER[1:]):
            settle_copy(i, k, moved(k, x=r, zh=p)).start()
        settle_own.start()

    def settled():
        for i, (r, p) in enumerate(ORDER[1:]):
            settle_copy(i, moved(k, x=-r, zh=p), moved(k, x=r, zh=p)).wait_recv()
        settle_own.wait()

    wg.s5()
    for r, p in ORDER:
        wg.recv_sibling(r, p)

    cos_sin = (cosine, sine)

    def project(h):
        first = h * part_rows

        def block(step, carry):
            if h == 1:

                @pl.when(step == 5)
                def _():
                    xg[1].s4()

                @pl.when(step == 7)
                def _():
                    kg[0].s1()
                    kg[0].s2()
                    xg[1].s5()
                    settle()

            dx = pick(step, [r % 4 for r, _ in ORDER])
            dz = pick(step, [p for _, p in ORDER])
            t = ((k["zh"] + dz) % 2) * 4 + (k["x"] + dx) % 4
            g = gain[t]
            for i in range(part_rows // 128):
                r = pl.ds(first + i * 128, 128)
                inv = inverse[r, :]
                for j in range(x_all.shape[2] // 128):
                    piece = x_all[t, r, pl.ds(j * 128, 128)].astype(F32)
                    normed[pl.ds(i * 128, 128), pl.ds(j * 128, 128)] = (
                        piece * inv * g[:, j * 128 : (j + 1) * 128]
                    ).astype(BF16)
            part = jnp.dot(normed[:, 0:wrows], w_all[2 * t], preferred_element_type=F32)
            part = part + jnp.dot(
                normed[:, wrows : 2 * wrows], w_all[2 * t + 1], preferred_element_type=F32
            )
            acc[first : first + part_rows, :] += part
            return carry

        lax.fori_loop(0, 8, block, 0)
        r = slice(first, first + part_rows)
        cos, sin = (x[r, :] for x in cos_sin)

        def turned(head):
            u = acc[r, head * HD : (head + 1) * HD] + bias[:, head * HD : (head + 1) * HD]
            return (u * cos + pltpu.roll(u, HD // 2, 1) * sin).astype(BF16)

        own = kv_rows(h, k)
        kv_all[own, 0:HD] = turned(heads)
        kv_all[own, HD : 2 * HD] = (acc[r, qc + kc :] + bias[:, qc + kc :]).astype(BF16)
        for head in range(heads):
            q[head, r, :] = turned(head)

    xg[0].s5()
    project(0)
    kg[0].s0()
    project(1)
    kg[1].s0()

    factor = HD ** (-0.5) / math.log(2.0)
    keys = 2 * rows
    tiles = rows // QT
    events = {}

    def event(step, *fns):
        events.setdefault(step, []).extend(fns)

    def sib(h, r):
        return lambda: (kg[h].recv_sibling(r, 0), kg[h].recv_sibling(r, 1))

    def close(i):
        f, n = CHUNKS[i]
        r = pl.ds(f * QT, n * QT)
        for h in range(heads):
            bottom = jnp.sum(low[h, r, :], -1, keepdims=True)
            done = (num[h, r, :] / bottom).astype(BF16)
            ctx_all[r, pl.ds(pl.multiple_of(me_t * cw + h * HD, HD), HD)] = done

    def send_ctx(i):
        cg[i].s0()

    def settle_sends():
        for i, (r, p) in enumerate(ORDER[1:]):
            spread_copy(i, k, moved(k, y=r, zl=p)).wait_send()
            settle_copy(i, k, moved(k, x=r, zh=p)).wait_send()
            ssq_copy(i, k, moved(k, x=r, zh=p)).wait_send()
        for i, (r, p, c) in enumerate(s_list):
            pos_copy(i, k, moved(k, y=r, zl=p, c=c)).wait_send()
        for x in [*xg, wg]:
            x.finish()

    def ctx_last(i):
        cg[i].s4()
        cg[i].s5()

    event(0, sib(0, 0))
    event(2, kg[0].s3, kg[0].s4, sib(0, -1))
    event(3, kg[1].s1, kg[1].s2, sib(0, 1))
    event(4, settled, og.s0_ring, sib(1, 0), kg[0].s5)
    event(5, kg[1].s3, og.s0_pair, sib(0, 2))
    event(6, kg[1].s4, sib(1, -1))
    event(7, sib(1, 1), settle_sends)
    event(8, kg[1].s5, sib(1, 2))
    event(9, lambda: close(0), lambda: send_ctx(0))
    event(11, og.s1)
    event(13, og.s2, cg[0].s1, lambda: close(1), lambda: send_ctx(1))
    event(14, cg[0].s2, og.s3)
    event(15, cg[0].s3)

    def dispatch(g, first, last):
        if last - first == 1:
            for fn in events.get(first, []):
                fn()
            return
        middle = (first + last) // 2
        lax.cond(
            g < middle, lambda: dispatch(g, first, middle), lambda: dispatch(g, middle, last)
        )

    def step(g, carry):
        dispatch(g, 0, 4 * tiles)
        units = [Unit(2 * g + half, u) for half in range(2) for u in range(heads // GROUP)]
        s, held = units[0].scores(), None
        for i, unit in enumerate(units):
            later = units[i + 1].scores() if i + 1 < len(units) else None
            now = unit.soften(s)
            if held is not None:
                units[i - 1].collect(*held)
            s, held = later, now
        units[-1].collect(*held)
        return carry

    class Unit:
        def __init__(self, g, u):
            late = jnp.maximum(g - 18, 0)
            mid = jnp.maximum(g - 4, 0)
            kb = jnp.where(g < 4, 0, jnp.where(g < 18, 1 + mid // 2, 1 + late % 7))
            tile = jnp.where(g < 4, g, jnp.where(g < 18, mid % 2, 2 + late // 7))
            dy = pick(kb, [r % 4 for r, _ in ORDER])
            dz = pick(kb, [p for _, p in ORDER])
            self.block = dz * 4 + (k["y"] + dy) % 4
            self.kr = pl.ds(pl.multiple_of(self.block * keys, keys), keys)
            self.at = (slice(u * GROUP, (u + 1) * GROUP), pl.ds(pl.multiple_of(tile * QT, QT), QT), slice(None))
            self.mine = jnp.concatenate([own_pos[self.at[1], :]] * GROUP, 0)

        def scores(self):
            return lax.dot_general(
                q[self.at].reshape(GROUP * QT, HD), kv_all[self.kr, 0:HD], (((1,), (1,)), ((), ())),
                preferred_element_type=F32,
            )

        def soften(self, s):
            parts = []
            for j in range(keys // 128):
                lane = (j % (part_rows // 128)) * 128
                kp = key_pos[self.block * 4 + j // (part_rows // 128), :, lane : lane + 128]
                parts.append(jnp.where(kp <= self.mine, s[:, j * 128 : (j + 1) * 128], NEG_FILL))
            best = parts[0]
            for x in parts[1:]:
                best = jnp.maximum(best, x)
            old = top[self.at].reshape(GROUP * QT, 128)
            new = jnp.maximum(old, jnp.max(best, -1, keepdims=True))
            top[self.at] = new.reshape(GROUP, QT, 128)
            alpha = jnp.exp2((old - new) * factor)
            weights, total = [], low[self.at].reshape(GROUP * QT, 128) * alpha
            for x in parts:
                w = jnp.exp2((x - new) * factor)
                total = total + w
                weights.append(w.astype(BF16))
            low[self.at] = total.reshape(GROUP, QT, 128)
            return alpha, jnp.concatenate(weights, 1)

        def collect(self, alpha, weights):
            out = num[self.at].reshape(GROUP * QT, HD) * alpha + jnp.dot(
                weights, kv_all[self.kr, HD : 2 * HD], preferred_element_type=F32
            )
            num[self.at] = out.reshape(GROUP, QT, HD)

    lax.fori_loop(0, 4 * tiles, step, 0)

    close(2)
    send_ctx(2)
    def output(first, count):
        r = pl.ds(first * QT, count * QT)

        def part(c, carry):
            cols = pl.ds(pl.multiple_of(c * 256, 256), 256)
            w = wo_all[:, :, :, cols].reshape(ctx_all.shape[1], 256)
            summed = jnp.dot(ctx_all[r, :], w, preferred_element_type=F32)
            mixed_v[r, cols] = (x_all[me_t, r, cols].astype(F32) + summed).astype(BF16)
            return carry

        lax.fori_loop(0, mixed.shape[1] // 256, part, 0)
        c = pltpu.make_async_copy(mixed_v.at[r], mixed.at[r], local_sem.at[6 + first])
        c.start()
        return c

    put = pltpu.make_async_copy(
        ctx_all.at[:, pl.ds(pl.multiple_of(me_t * cw, cw), cw)], context, local_sem.at[5]
    )
    put.start()
    kg[0].finish()
    kg[1].finish()
    cg[1].s1()
    cg[1].s2()
    cg[0].s4()
    cg[1].s3()
    cg[2].s1()
    og.s4()
    cg[2].s2()
    cg[0].s5()
    cg[2].s3()
    ctx_last(1)
    og.s5()
    for r, p in ORDER:
        og.recv_sibling(r, p)
    puts = [put, output(0, 2)]
    ctx_last(2)
    puts.append(output(2, 2))
    for x in [og, *cg]:
        x.finish()
    for c in puts:
        c.wait()


def shards(tokens, positions, norm_gain, w_query, w_key, w_value, b_query, b_key, b_value, w_out):
    rows, feats = tokens.shape
    qc, kc = w_query.shape[1], w_key.shape[1]
    wrows = w_query.shape[0]
    heads = qc // HD
    nt, ns = lax.axis_size("tensor"), lax.axis_size("seq")
    half = HD // 2
    inv_freq = ROPE_BASE ** (-jnp.arange(half, dtype=F32) * 2.0 / HD)
    angles = positions.astype(F32)[:, None] * inv_freq[None, :]
    cos, sin = jnp.cos(angles), jnp.sin(angles)
    cosine = jnp.concatenate([cos, cos], 1)
    sine = jnp.concatenate([-sin, sin], 1)
    bias = jnp.concatenate((b_query, b_key, b_value))[None, :]
    pos = jnp.pad(positions.astype(F32).reshape(rows // 128, 128), ((0, 8 - rows // 128), (0, 0)))
    any_, vmem = pl.BlockSpec(memory_space=pltpu.HBM), pl.BlockSpec(memory_space=pltpu.VMEM)
    dma = pltpu.SemaphoreType.DMA
    return pl.pallas_call(
        block_kernel,
        name="block",
        out_shape=(
            jax.ShapeDtypeStruct((rows, feats), BF16),
            jax.ShapeDtypeStruct((rows, qc), BF16),
        ),
        in_specs=[any_, any_, vmem, any_, any_, any_, vmem, vmem, vmem, any_],
        out_specs=(pl.BlockSpec(memory_space=pl.ANY), pl.BlockSpec(memory_space=pl.ANY)),
        scratch_shapes=[
            pltpu.VMEM((nt, rows, feats), BF16),
            pltpu.VMEM((ns, wrows, qc + 2 * kc), BF16),
            pltpu.VMEM((rows, qc + 2 * kc), F32),
            pltpu.VMEM((rows // 2, feats), BF16),
            pltpu.VMEM((nt, 8, 128), F32),
            pltpu.VMEM((rows, 128), F32),
            pltpu.VMEM((nt, w_out.shape[0] // 8, w_out.shape[1]), BF16),
            pltpu.VMEM((ns, 8, 128), F32),
            pltpu.VMEM((heads, rows, HD), BF16),
            pltpu.VMEM((ns * rows, 2 * HD), BF16),
            pltpu.VMEM((nt, 8, qc // 8, feats), BF16),
            pltpu.VMEM((rows, nt * qc), BF16),
            pltpu.VMEM((2 * ns, 1, rows // 2), F32),
            pltpu.VMEM((rows, 128), F32),
            pltpu.VMEM((heads, rows, 128), F32),
            pltpu.VMEM((heads, rows, 128), F32),
            pltpu.VMEM((heads, rows, HD), F32),
            pltpu.VMEM((rows, feats), BF16),
            dma((10,)), dma((40,)), dma((40,)), dma((20,)), dma((20,)),
            dma((8,)), dma((8,)), dma((16,)), dma((16,)), dma((16,)), dma((16,)),
            dma((40,)), dma((40,)), dma((20,)), dma((20,)), dma((48,)), dma((48,)),
        ],
        compiler_params=pltpu.CompilerParams(
            collective_id=0, has_side_effects=True, vmem_limit_bytes=50 * 1024 * 1024
        ),
    )(tokens, pos, norm_gain.reshape(nt, 1, feats), w_query, w_key, w_value, bias, cosine, sine, w_out)


def solution(mesh):
    in_specs = (
        P("seq", "tensor"),
        P("seq"),
        P(),
        P("seq", "tensor"),
        P("seq", "tensor"),
        P("seq", "tensor"),
        P("tensor"),
        P("tensor"),
        P("tensor"),
        P("tensor", "seq"),
    )
    out_specs = (P("seq", "tensor"), P("seq", "tensor"))
    return jax.shard_map(shards, mesh=mesh, in_specs=in_specs, out_specs=out_specs, check_vma=False)
```

```python
import functools
import math

import jax
import jax.numpy as jnp
import numpy as np
from jax import lax
from jax.experimental import pallas as pl
from jax.experimental.pallas import tpu as pltpu
from jax.sharding import PartitionSpec as P

HD = 128
NORM_EPS = 1e-06
ROPE_BASE = 1000000.0
NEG_FILL = -1e30
MESH = pl.DeviceIdType.MESH
BF16 = jnp.bfloat16
F32 = jnp.float32


def coords():
    s, t = lax.axis_index("seq"), lax.axis_index("tensor")
    return dict(y=s // 4, zl=(s // 2) % 2, c=s % 2, zh=t // 4, x=t % 4)


SIZES = dict(y=4, zl=2, c=2, zh=2, x=4)


def moved(k, **shift):
    k = dict(k)
    for name, by in shift.items():
        k[name] = (k[name] + (by + SIZES[name])) % SIZES[name]
    return k


def seq_of(k):
    return k["y"] * 4 + k["zl"] * 2 + k["c"]


def tensor_of(k):
    return k["zh"] * 4 + k["x"]


def device(k):
    return (seq_of(k), tensor_of(k))


SHARING = (0, 1, 2, 3, 4, 5, 6, 7, 8, 9, 10, 11, 13, 14, 15, 16, 17)
ALONE = (0, 1, 2, 4, 6, 8, 9, 13, 14, 15)


class Gather:
    def __init__(self, k, slot, half_rows, ring, pair, sibling, ssem, rsem, base=0, along=0, far_by_pair=False):
        self.k, self.slot, self.half = k, slot, half_rows
        self.ring, self.pair, self.sibling = ring, pair, sibling
        self.ssem, self.rsem, self.base = ssem, rsem, base
        self.along, self.direct = along, 2 * half_rows - 2 * along
        self.far_by_pair = far_by_pair or not sibling
        self.used = SHARING if sibling else ALONE
        self.sent = []

    def at(self, r=0, p=0, c=0):
        return (r, p, c)

    def place(self, where):
        r, p, c = where
        return moved(self.k, **{self.ring: r, self.pair: p, "c": c})

    def copy(self, i, block, target, half):
        ref = self.slot(self.place(block))
        if half is not None:
            first, count = half if isinstance(half, tuple) else (half * self.half, self.half)
            ref = ref.at[pl.ds(first, count)]
        return pltpu.make_async_remote_copy(
            src_ref=ref,
            dst_ref=ref,
            send_sem=self.ssem.at[self.base + self.used.index(i)],
            recv_sem=self.rsem.at[self.base + self.used.index(i)],
            device_id=device(self.place(target)),
            device_id_type=MESH,
        )

    def send(self, i, block, target, half=None):
        self.copy(i, block, target, half).start()
        self.sent.append((i, block, target, half))

    def recv(self, i, block, half=None):
        self.copy(i, block, (0, 0, 1) if self.sibling else (1, 0, 0), half).wait_recv()

    def share(self, i, block):
        if self.sibling:
            self.send(i, block, self.at(c=1))

    def s0(self):
        self.s0_ring()
        self.s0_pair()

    def s0_ring(self):
        self.send(0, self.at(), self.at(1))
        self.send(1, self.at(), self.at(-1))
        self.share(3, self.at())

    def s0_pair(self):
        self.send(2, self.at(), self.at(p=1))

    def s1(self):
        self.recv(0, self.at(-1))
        self.send(4, self.at(-1), self.at(1), 0)
        self.share(5, self.at(-1))
        self.recv(1, self.at(1))
        self.send(6, self.at(1), self.at(-1), 1)
        self.share(7, self.at(1))

    def s2(self):
        self.recv(2, self.at(p=1))
        self.send(8, self.at(p=1), self.at(1))
        self.send(9, self.at(p=1), self.at(-1))
        self.share(10, self.at(p=1))

    def s3(self):
        self.recv(4, self.at(2), 0)
        self.recv(6, self.at(2), 1)
        self.share(11, self.at(2))
        if self.far_by_pair:
            self.send(13, self.at(2), self.at(p=1), (0, self.direct))

    def s4(self):
        self.recv(8, self.at(-1, 1))
        if not self.far_by_pair:
            self.send(13, self.at(-1, 1), self.at(1), 0)
        elif self.along:
            self.send(14, self.at(-1, 1), self.at(1), (self.direct, self.along))
        self.share(14, self.at(-1, 1))
        self.recv(9, self.at(1, 1))
        if not self.far_by_pair:
            self.send(15, self.at(1, 1), self.at(-1), 1)
        elif self.along:
            self.send(15, self.at(1, 1), self.at(-1), (self.direct + self.along, self.along))
        self.share(16, self.at(1, 1))

    def s5(self):
        if self.far_by_pair:
            self.recv(13, self.at(2, 1), (0, self.direct))
            if self.along:
                self.recv(14, self.at(2, 1), (self.direct, self.along))
                self.recv(15, self.at(2, 1), (self.direct + self.along, self.along))
        else:
            self.recv(13, self.at(2, 1), 0)
            self.recv(15, self.at(2, 1), 1)
        self.share(17, self.at(2, 1))

    SHARED = {(0, 0): 3, (-1, 0): 5, (1, 0): 7, (0, 1): 10, (2, 0): 11, (-1, 1): 14, (1, 1): 16, (2, 1): 17}

    def recv_sibling(self, r, p):
        self.recv(self.SHARED[(r, p)], self.at(r, p, 1))

    def finish(self):
        for i, block, target, half in self.sent:
            self.copy(i, block, target, half).wait_send()


ORDER = ((0, 0), (-1, 0), (1, 0), (0, 1), (2, 0), (-1, 1), (1, 1), (2, 1))


def pick(index, values):
    out = values[0]
    for i, v in enumerate(values[1:], 1):
        out = jnp.where(index == i, v, out)
    return out


def greet(k, peers):
    barrier = pltpu.get_barrier_semaphore()
    for p in peers:
        pl.semaphore_signal(barrier, inc=1, device_id=device(p), device_id_type=MESH)
    pl.semaphore_wait(barrier, len(peers))


def tensor_peers(k):
    return [moved(k, x=r, zh=p) for r, p in ORDER[1:]]


def seq_peers(k):
    return [
        moved(k, y=r, zl=p, c=c) for r, p in ORDER for c in (0, 1) if (r, p, c) != (0, 0, 0)
    ]


def as_columns(rows):
    parts = [jnp.broadcast_to(rows[i : i + 1, :], (128, 128)).T for i in range(rows.shape[0])]
    return jnp.concatenate(parts, 0)


QT = 128
CHUNKS = ((0, 2), (2, 1), (3, 1))
GROUP = 2
ALONG = (64, 0)


def block_kernel(
    tokens, pos, gain_in, w_query, w_key, w_value, b_query, b_key, b_value, freq_in, w_out,
    mixed, context, gain, bias, freq, cosine, sine,
    x_all, w_all, acc, normed, ssq, inverse, wo_mid, pos_all,
    q, kv_all, wo_all, ctx_all, key_pos, own_pos, top, low, num, mixed_v,
    local_sem, x_ssem, x_rsem, w_ssem, w_rsem, s_ssem, s_rsem, p_ssem, p_rsem, t_ssem, t_rsem,
    kv_ssem, kv_rsem, wo_ssem, wo_rsem, c_ssem, c_rsem, out_sem,
):
    k = coords()
    me_s, me_t = seq_of(k), tensor_of(k)
    rows = tokens.shape[0]
    qc, kc = w_query.shape[1], w_key.shape[1]
    wrows = w_query.shape[0]
    heads = qc // HD
    cw = qc

    loads = [
        pltpu.make_async_copy(tokens, x_all.at[me_t], local_sem.at[0]),
        pltpu.make_async_copy(w_query, w_all.at[me_s, :, pl.ds(0, qc)], local_sem.at[1]),
        pltpu.make_async_copy(w_key, w_all.at[me_s, :, pl.ds(qc, kc)], local_sem.at[2]),
        pltpu.make_async_copy(w_value, w_all.at[me_s, :, pl.ds(qc + kc, kc)], local_sem.at[3]),
        pltpu.make_async_copy(pos, pos_all.at[me_s], local_sem.at[4]),
        pltpu.make_async_copy(gain_in, gain, local_sem.at[6]),
        pltpu.make_async_copy(b_query, bias.at[:, pl.ds(0, qc)], local_sem.at[7]),
        pltpu.make_async_copy(b_key, bias.at[:, pl.ds(qc, kc)], local_sem.at[8]),
        pltpu.make_async_copy(b_value, bias.at[:, pl.ds(qc + kc, kc)], local_sem.at[9]),
        pltpu.make_async_copy(freq_in, freq, local_sem.at[10]),
    ]
    for c in loads:
        c.start()
    greet(k, tensor_peers(k) + seq_peers(k))
    for c in loads:
        c.wait()

    def wo_slot(b):
        return wo_all.at[:, seq_of(b) // 2, :, pl.ds(pl.multiple_of(b["c"] * cw, cw), cw)]

    def ctx_slot(first, count):
        return lambda b: ctx_all.at[
            pl.ds(first * QT, count * QT), pl.ds(pl.multiple_of(tensor_of(b) * cw, cw), cw)
        ]

    part_rows = rows // 2
    xg = [
        Gather(
            k, lambda b, h=h: x_all.at[tensor_of(b), pl.ds(h * part_rows, part_rows)], part_rows // 2,
            "x", "zh", False, x_ssem, x_rsem, base=10 * h, along=ALONG[h],
        )
        for h in range(2)
    ]
    wg = Gather(k, lambda b: w_all.at[seq_of(b)], wrows // 2, "y", "zl", True, w_ssem, w_rsem)
    def kv_rows(h, b):
        return pl.ds(pl.multiple_of((h * 16 + seq_of(b)) * part_rows, part_rows), part_rows)

    kg = [
        Gather(
            k, lambda b, h=h: kv_all.at[kv_rows(h, b)], part_rows // 2, "y", "zl", True,
            kv_ssem, kv_rsem, base=17 * h, far_by_pair=h == 1,
        )
        for h in range(2)
    ]
    og = Gather(
        k, wo_slot, wo_all.shape[0] // 2, "y", "zl", True, wo_ssem, wo_rsem
    )
    cg = [
        Gather(k, ctx_slot(f, n), n * QT // 2, "x", "zh", False, c_ssem, c_rsem, base=8 * i)
        for i, (f, n) in enumerate(CHUNKS)
    ]

    eighth = wo_mid.shape[1]

    def spread_copy(i, source, target):
        return pltpu.make_async_remote_copy(
            w_out.at[pl.ds((seq_of(target) // 2) * eighth, eighth)], wo_mid.at[seq_of(source) // 2],
            t_ssem.at[i], t_rsem.at[i], device_id=device(target), device_id_type=MESH,
        )

    def wo_part(t):
        return wo_all.at[t, me_s // 2, :, pl.ds(pl.multiple_of(k["c"] * cw, cw), cw)]

    def settle_copy(i, source, target):
        return pltpu.make_async_remote_copy(
            wo_mid.at[tensor_of(target)], wo_part(tensor_of(source)),
            t_ssem.at[8 + i], t_rsem.at[8 + i], device_id=device(target), device_id_type=MESH,
        )

    spread_own = pltpu.make_async_copy(
        w_out.at[pl.ds((me_s // 2) * eighth, eighth)], wo_mid.at[me_s // 2], t_ssem.at[7]
    )
    settle_own = pltpu.make_async_copy(wo_mid.at[me_t], wo_part(me_t), t_ssem.at[15])

    def pos_copy(i, b, target):
        ref = pos_all.at[seq_of(b)]
        return pltpu.make_async_remote_copy(
            ref, ref, p_ssem.at[i], p_rsem.at[i], device_id=device(target), device_id_type=MESH
        )

    s_list = [(r, p, c) for r, p in ORDER for c in (0, 1) if (r, p, c) != (0, 0, 0)]

    def ssq_copy(i, b, target):
        ref = ssq.at[tensor_of(b)]
        return pltpu.make_async_remote_copy(
            ref, ref, s_ssem.at[i], s_rsem.at[i], device_id=device(target), device_id_type=MESH
        )

    wg.s0()
    xg[0].s0_ring()
    xg[1].s0_ring()
    for i in range(rows // 128):
        xb = x_all[me_t, pl.ds(i * 128, 128), :].astype(F32)
        total = jnp.sum(xb * xb, -1, keepdims=True)
        ssq[me_t, i : i + 1, :] = jnp.broadcast_to(total, (128, 128)).T[0:1, :]
    for i, (r, p, c) in enumerate(s_list):
        pos_copy(i, k, moved(k, y=r, zl=p, c=c)).start()
    acc[...] = jnp.zeros_like(acc)
    top[...] = jnp.full_like(top, NEG_FILL)
    low[...] = jnp.zeros_like(low)
    num[...] = jnp.zeros_like(num)
    for i, (r, p) in enumerate(ORDER[1:]):
        ssq_copy(i, k, moved(k, x=r, zh=p)).start()

    wg.s1()
    wg.s2()
    xg[0].s0_pair()
    xg[0].s1()
    xg[1].s1()
    for i, (r, p) in enumerate(ORDER[1:]):
        ssq_copy(i, moved(k, x=-r, zh=p), k).wait_recv()
    total = ssq[0]
    for i in range(1, 8):
        total = total + ssq[i]
    scale = lax.rsqrt(total / (8 * x_all.shape[2]) + NORM_EPS)
    inverse[...] = as_columns(scale[0 : rows // 128, :])
    wg.s3()
    xg[0].s3()
    xg[1].s0_pair()
    xg[0].s2()
    xg[1].s3()
    wg.s4()
    for i, (r, p) in enumerate(ORDER[1:]):
        spread_copy(i, k, moved(k, y=r, zl=p)).start()
    spread_own.start()
    xg[0].s4()
    xg[1].s2()
    for i, (r, p, c) in enumerate(s_list):
        pos_copy(i, moved(k, y=-r, zl=p, c=c), k).wait_recv()

    def spread(s, carry):
        for h in range(2):
            for j in range(part_rows // 128):
                row = h * (part_rows // 128) + j
                key_pos[h * 16 + s, :, j * 128 : (j + 1) * 128] = pos_all[s, row : row + 1, :].astype(F32)
        return carry

    lax.fori_loop(0, pos_all.shape[0], spread, 0)
    own_pos[...] = as_columns(pos_all[me_s].astype(F32))
    lane = lax.broadcasted_iota(jnp.int32, (128, HD), 1)
    for i in range(rows // 128):
        r = slice(i * 128, (i + 1) * 128)
        angles = own_pos[r, :] * freq[...]
        cosine[r, :] = jnp.cos(angles)
        turn = jnp.sin(angles)
        sine[r, :] = jnp.where(lane < HD // 2, -turn, turn)
    def settle():
        for i, (r, p) in enumerate(ORDER[1:]):
            spread_copy(i, moved(k, y=-r, zl=p), moved(k, y=r, zl=p)).wait_recv()
        spread_own.wait()
        for i, (r, p) in enumerate(ORDER[1:]):
            settle_copy(i, k, moved(k, x=r, zh=p)).start()
        settle_own.start()

    def settled():
        for i, (r, p) in enumerate(ORDER[1:]):
            settle_copy(i, moved(k, x=-r, zh=p), moved(k, x=r, zh=p)).wait_recv()
        settle_own.wait()

    wg.s5()
    for r, p in ORDER:
        wg.recv_sibling(r, p)

    cos_sin = (cosine, sine)

    def project(h):
        first = h * part_rows

        def block(step, carry):
            if h == 1:

                @pl.when(step == 5)
                def _():
                    xg[1].s4()

                @pl.when(step == 7)
                def _():
                    kg[0].s1()
                    kg[0].s2()
                    xg[1].s5()
                    settle()

            dx = pick(step, [r % 4 for r, _ in ORDER])
            dz = pick(step, [p for _, p in ORDER])
            t = ((k["zh"] + dz) % 2) * 4 + (k["x"] + dx) % 4
            g = gain[t]
            for i in range(part_rows // 128):
                r = pl.ds(first + i * 128, 128)
                inv = inverse[r, :]
                for j in range(x_all.shape[2] // 128):
                    piece = x_all[t, r, pl.ds(j * 128, 128)].astype(F32)
                    normed[pl.ds(i * 128, 128), pl.ds(j * 128, 128)] = (
                        piece * inv * g[:, j * 128 : (j + 1) * 128]
                    ).astype(BF16)
            part = jnp.dot(normed[:, 0:wrows], w_all[2 * t], preferred_element_type=F32)
            part = part + jnp.dot(
                normed[:, wrows : 2 * wrows], w_all[2 * t + 1], preferred_element_type=F32
            )
            acc[first : first + part_rows, :] += part
            return carry

        lax.fori_loop(0, 8, block, 0)
        r = slice(first, first + part_rows)
        cos, sin = (x[r, :] for x in cos_sin)

        def turned(head):
            u = acc[r, head * HD : (head + 1) * HD] + bias[:, head * HD : (head + 1) * HD]
            return (u * cos + pltpu.roll(u, HD // 2, 1) * sin).astype(BF16)

        own = kv_rows(h, k)
        kv_all[own, 0:HD] = turned(heads)
        kv_all[own, HD : 2 * HD] = (acc[r, qc + kc :] + bias[:, qc + kc :]).astype(BF16)
        for head in range(heads):
            q[head, r, :] = turned(head)

    xg[0].s5()
    project(0)
    kg[0].s0()
    project(1)
    kg[1].s0()

    factor = HD ** (-0.5) / math.log(2.0)
    keys = 2 * rows
    tiles = rows // QT
    events = {}

    def event(step, *fns):
        events.setdefault(step, []).extend(fns)

    def sib(h, r):
        return lambda: (kg[h].recv_sibling(r, 0), kg[h].recv_sibling(r, 1))

    def close(i):
        f, n = CHUNKS[i]
        r = pl.ds(f * QT, n * QT)
        for h in range(heads):
            bottom = jnp.sum(low[h, r, :], -1, keepdims=True)
            done = (num[h, r, :] / bottom).astype(BF16)
            ctx_all[r, pl.ds(pl.multiple_of(me_t * cw + h * HD, HD), HD)] = done

    def send_ctx(i):
        cg[i].s0()

    def settle_sends():
        for i, (r, p) in enumerate(ORDER[1:]):
            spread_copy(i, k, moved(k, y=r, zl=p)).wait_send()
            settle_copy(i, k, moved(k, x=r, zh=p)).wait_send()
            ssq_copy(i, k, moved(k, x=r, zh=p)).wait_send()
        for i, (r, p, c) in enumerate(s_list):
            pos_copy(i, k, moved(k, y=r, zl=p, c=c)).wait_send()
        for x in [*xg, wg]:
            x.finish()

    def ctx_last(i):
        cg[i].s4()
        cg[i].s5()

    event(0, sib(0, 0))
    event(2, kg[0].s3, kg[0].s4, sib(0, -1))
    event(3, kg[1].s1, kg[1].s2, sib(0, 1))
    event(4, settled, og.s0_ring, sib(1, 0), kg[0].s5)
    event(5, kg[1].s3, og.s0_pair, sib(0, 2))
    event(6, kg[1].s4, sib(1, -1))
    event(7, sib(1, 1), settle_sends)
    event(8, kg[1].s5, sib(1, 2))
    event(9, lambda: close(0), lambda: send_ctx(0))
    event(11, og.s1)
    event(13, cg[0].s1, lambda: close(1), lambda: send_ctx(1), og.s2)
    event(14, cg[0].s2)
    event(15, cg[0].s3, og.s3)

    def dispatch(g, first, last):
        if last - first == 1:
            for fn in events.get(first, []):
                fn()
            return
        middle = (first + last) // 2
        lax.cond(
            g < middle, lambda: dispatch(g, first, middle), lambda: dispatch(g, middle, last)
        )

    def step(g, carry):
        dispatch(g, 0, 4 * tiles)
        units = [Unit(2 * g + half, u) for half in range(2) for u in range(heads // GROUP)]
        s, held = units[0].scores(), None
        for i, unit in enumerate(units):
            later = units[i + 1].scores() if i + 1 < len(units) else None
            now = unit.soften(s)
            if held is not None:
                units[i - 1].collect(*held)
            s, held = later, now
        units[-1].collect(*held)
        return carry

    class Unit:
        def __init__(self, g, u):
            late = jnp.maximum(g - 18, 0)
            mid = jnp.maximum(g - 4, 0)
            kb = jnp.where(g < 4, 0, jnp.where(g < 18, 1 + mid // 2, 1 + late % 7))
            tile = jnp.where(g < 4, g, jnp.where(g < 18, mid % 2, 2 + late // 7))
            dy = pick(kb, [r % 4 for r, _ in ORDER])
            dz = pick(kb, [p for _, p in ORDER])
            self.block = dz * 4 + (k["y"] + dy) % 4
            self.kr = pl.ds(pl.multiple_of(self.block * keys, keys), keys)
            self.at = (slice(u * GROUP, (u + 1) * GROUP), pl.ds(pl.multiple_of(tile * QT, QT), QT), slice(None))
            self.mine = jnp.concatenate([own_pos[self.at[1], :]] * GROUP, 0)

        def scores(self):
            return lax.dot_general(
                q[self.at].reshape(GROUP * QT, HD), kv_all[self.kr, 0:HD], (((1,), (1,)), ((), ())),
                preferred_element_type=F32,
            )

        def soften(self, s):
            parts = []
            for j in range(keys // 128):
                lane = (j % (part_rows // 128)) * 128
                kp = key_pos[self.block * 4 + j // (part_rows // 128), :, lane : lane + 128]
                parts.append(jnp.where(kp <= self.mine, s[:, j * 128 : (j + 1) * 128], NEG_FILL))
            best = parts[0]
            for x in parts[1:]:
                best = jnp.maximum(best, x)
            old = top[self.at].reshape(GROUP * QT, 128)
            new = jnp.maximum(old, jnp.max(best, -1, keepdims=True))
            top[self.at] = new.reshape(GROUP, QT, 128)
            alpha = jnp.exp2((old - new) * factor)
            weights, total = [], low[self.at].reshape(GROUP * QT, 128) * alpha
            for x in parts:
                w = jnp.exp2((x - new) * factor)
                total = total + w
                weights.append(w.astype(BF16))
            low[self.at] = total.reshape(GROUP, QT, 128)
            return alpha, jnp.concatenate(weights, 1)

        def collect(self, alpha, weights):
            out = num[self.at].reshape(GROUP * QT, HD) * alpha + jnp.dot(
                weights, kv_all[self.kr, HD : 2 * HD], preferred_element_type=F32
            )
            num[self.at] = out.reshape(GROUP, QT, HD)

    lax.fori_loop(0, 4 * tiles, step, 0)

    close(2)
    send_ctx(2)
    def output(first, count):
        r = pl.ds(first * QT, count * QT)

        def put_part(c):
            cols = pl.ds(pl.multiple_of(c * 256, 256), 256)
            return pltpu.make_async_copy(mixed_v.at[r, cols], mixed.at[r, cols], out_sem.at[0, c])

        def part(c, carry):
            cols = pl.ds(pl.multiple_of(c * 256, 256), 256)
            w = wo_all[:, :, :, cols].reshape(ctx_all.shape[1], 256)
            summed = jnp.dot(ctx_all[r, :], w, preferred_element_type=F32)
            mixed_v[r, cols] = (x_all[me_t, r, cols].astype(F32) + summed).astype(BF16)
            put_part(c).start()
            return carry

        lax.fori_loop(0, mixed.shape[1] // 256, part, 0)
        return [put_part(c) for c in range(mixed.shape[1] // 256)]

    put = pltpu.make_async_copy(
        ctx_all.at[:, pl.ds(pl.multiple_of(me_t * cw, cw), cw)], context, local_sem.at[5]
    )
    put.start()
    kg[0].finish()
    kg[1].finish()
    cg[1].s1()
    cg[1].s2()
    cg[0].s4()
    og.s4()
    cg[1].s3()
    cg[2].s1()
    cg[2].s2()
    cg[0].s5()
    cg[2].s3()
    ctx_last(1)
    og.s5()
    for r, p in ORDER:
        og.recv_sibling(r, p)
    ctx_last(2)
    puts = [put, *output(0, 4)]
    for x in [og, *cg]:
        x.finish()
    for c in puts:
        c.wait()


def shards(tokens, positions, norm_gain, w_query, w_key, w_value, b_query, b_key, b_value, w_out):
    rows, feats = tokens.shape
    qc, kc = w_query.shape[1], w_key.shape[1]
    wrows = w_query.shape[0]
    heads = qc // HD
    nt, ns = lax.axis_size("tensor"), lax.axis_size("seq")
    inv_freq = ROPE_BASE ** (-np.arange(HD // 2, dtype=np.float64) * 2.0 / HD)
    freq = jnp.asarray(np.concatenate([inv_freq, inv_freq])[None, :].astype(np.float32))
    hbm = pl.BlockSpec(memory_space=pltpu.HBM)
    dma = pltpu.SemaphoreType.DMA
    return pl.pallas_call(
        block_kernel,
        name="block",
        out_shape=(
            jax.ShapeDtypeStruct((rows, feats), BF16),
            jax.ShapeDtypeStruct((rows, qc), BF16),
        ),
        in_specs=[hbm] * 11,
        out_specs=(pl.BlockSpec(memory_space=pl.ANY), pl.BlockSpec(memory_space=pl.ANY)),
        scratch_shapes=[
            pltpu.VMEM((nt, 1, feats), F32),
            pltpu.VMEM((1, qc + 2 * kc), F32),
            pltpu.VMEM((1, HD), F32),
            pltpu.VMEM((rows, HD), F32),
            pltpu.VMEM((rows, HD), F32),
            pltpu.VMEM((nt, rows, feats), BF16),
            pltpu.VMEM((ns, wrows, qc + 2 * kc), BF16),
            pltpu.VMEM((rows, qc + 2 * kc), F32),
            pltpu.VMEM((rows // 2, feats), BF16),
            pltpu.VMEM((nt, 8, 128), F32),
            pltpu.VMEM((rows, 128), F32),
            pltpu.VMEM((nt, w_out.shape[0] // 8, w_out.shape[1]), BF16),
            pltpu.VMEM((ns, rows // 128, 128), jnp.int32),
            pltpu.VMEM((heads, rows, HD), BF16),
            pltpu.VMEM((ns * rows, 2 * HD), BF16),
            pltpu.VMEM((nt, 8, qc // 8, feats), BF16),
            pltpu.VMEM((rows, nt * qc), BF16),
            pltpu.VMEM((2 * ns, 1, rows // 2), F32),
            pltpu.VMEM((rows, 128), F32),
            pltpu.VMEM((heads, rows, 128), F32),
            pltpu.VMEM((heads, rows, 128), F32),
            pltpu.VMEM((heads, rows, HD), F32),
            pltpu.VMEM((rows, feats), BF16),
            dma((12,)), dma((20,)), dma((20,)), dma((17,)), dma((17,)),
            dma((7,)), dma((7,)), dma((15,)), dma((15,)), dma((16,)), dma((15,)),
            dma((34,)), dma((34,)), dma((17,)), dma((17,)), dma((24,)), dma((24,)), dma((1, 4)),
        ],
        compiler_params=pltpu.CompilerParams(
            collective_id=0, has_side_effects=True, vmem_limit_bytes=58 * 1024 * 1024
        ),
    )(
        tokens, positions.reshape(rows // 128, 128), norm_gain.reshape(nt, 1, feats), w_query, w_key, w_value,
        b_query[None, :], b_key[None, :], b_value[None, :], freq, w_out,
    )


def solution(mesh):
    in_specs = (
        P("seq", "tensor"),
        P("seq"),
        P(),
        P("seq", "tensor"),
        P("seq", "tensor"),
        P("seq", "tensor"),
        P("tensor"),
        P("tensor"),
        P("tensor"),
        P("tensor", "seq"),
    )
    out_specs = (P("seq", "tensor"), P("seq", "tensor"))
    return jax.shard_map(shards, mesh=mesh, in_specs=in_specs, out_specs=out_specs, check_vma=False)
```

```python
import functools
import math

import jax
import jax.numpy as jnp
import numpy as np
from jax import lax
from jax.experimental import pallas as pl
from jax.experimental.pallas import tpu as pltpu
from jax.sharding import PartitionSpec as P

HD = 128
NORM_EPS = 1e-06
ROPE_BASE = 1000000.0
NEG_FILL = -1e30
MESH = pl.DeviceIdType.MESH
BF16 = jnp.bfloat16
F32 = jnp.float32


def coords():
    s, t = lax.axis_index("seq"), lax.axis_index("tensor")
    return dict(y=s // 4, zl=(s // 2) % 2, c=s % 2, zh=t // 4, x=t % 4)


SIZES = dict(y=4, zl=2, c=2, zh=2, x=4)


def moved(k, **shift):
    k = dict(k)
    for name, by in shift.items():
        k[name] = (k[name] + (by + SIZES[name])) % SIZES[name]
    return k


def seq_of(k):
    return k["y"] * 4 + k["zl"] * 2 + k["c"]


def tensor_of(k):
    return k["zh"] * 4 + k["x"]


def device(k):
    return (seq_of(k), tensor_of(k))


SHARING = (0, 1, 2, 3, 4, 5, 6, 7, 8, 9, 10, 11, 13, 14, 15, 16, 17, 18)
ALONE = (0, 1, 2, 4, 6, 8, 9, 13, 14, 15)


class Gather:
    def __init__(self, k, slot, half_rows, ring, pair, sibling, ssem, rsem, base=0, along=0, far_by_pair=False):
        self.k, self.slot, self.half = k, slot, half_rows
        self.ring, self.pair, self.sibling = ring, pair, sibling
        self.ssem, self.rsem, self.base = ssem, rsem, base
        self.along, self.direct = along, 2 * half_rows - 2 * along
        self.far_by_pair = far_by_pair or not sibling
        self.used = SHARING if sibling else ALONE
        self.sent = []

    def at(self, r=0, p=0, c=0):
        return (r, p, c)

    def place(self, where):
        r, p, c = where
        return moved(self.k, **{self.ring: r, self.pair: p, "c": c})

    def copy(self, i, block, target, half):
        ref = self.slot(self.place(block))
        if half is not None:
            first, count = half if isinstance(half, tuple) else (half * self.half, self.half)
            ref = ref.at[pl.ds(first, count)]
        return pltpu.make_async_remote_copy(
            src_ref=ref,
            dst_ref=ref,
            send_sem=self.ssem.at[self.base + self.used.index(i)],
            recv_sem=self.rsem.at[self.base + self.used.index(i)],
            device_id=device(self.place(target)),
            device_id_type=MESH,
        )

    def send(self, i, block, target, half=None):
        self.copy(i, block, target, half).start()
        self.sent.append((i, block, target, half))

    def recv(self, i, block, half=None):
        self.copy(i, block, (0, 0, 1) if self.sibling else (1, 0, 0), half).wait_recv()

    def share(self, i, block, half=None):
        if self.sibling:
            self.send(i, block, self.at(c=1), half)

    def s0(self):
        self.s0_ring()
        self.s0_pair()

    def s0_ring(self):
        self.send(0, self.at(), self.at(1))
        self.send(1, self.at(), self.at(-1))
        self.share(3, self.at())

    def s0_pair(self):
        self.send(2, self.at(), self.at(p=1))

    def s1(self):
        self.recv(0, self.at(-1))
        self.send(4, self.at(-1), self.at(1), 0)
        self.share(5, self.at(-1))
        self.recv(1, self.at(1))
        self.send(6, self.at(1), self.at(-1), 1)
        self.share(7, self.at(1))

    def s2(self):
        self.recv(2, self.at(p=1))
        self.send(8, self.at(p=1), self.at(1))
        self.send(9, self.at(p=1), self.at(-1))
        self.share(10, self.at(p=1))

    def s3(self):
        self.recv(4, self.at(2), 0)
        self.recv(6, self.at(2), 1)
        self.share(11, self.at(2))
        if self.far_by_pair:
            self.send(13, self.at(2), self.at(p=1), (0, self.direct))

    def s4(self):
        self.recv(8, self.at(-1, 1))
        if not self.far_by_pair:
            self.send(13, self.at(-1, 1), self.at(1), 0)
        elif self.along:
            self.send(14, self.at(-1, 1), self.at(1), (self.direct, self.along))
        self.share(14, self.at(-1, 1))
        self.recv(9, self.at(1, 1))
        if not self.far_by_pair:
            self.send(15, self.at(1, 1), self.at(-1), 1)
        elif self.along:
            self.send(15, self.at(1, 1), self.at(-1), (self.direct + self.along, self.along))
        self.share(16, self.at(1, 1))

    def s5(self):
        if self.far_by_pair:
            self.recv(13, self.at(2, 1), (0, self.direct))
            if self.along:
                self.recv(14, self.at(2, 1), (self.direct, self.along))
                self.recv(15, self.at(2, 1), (self.direct + self.along, self.along))
            self.share(17, self.at(2, 1))
        else:
            self.recv(13, self.at(2, 1), 0)
            self.share(17, self.at(2, 1), 0)
            self.recv(15, self.at(2, 1), 1)
            self.share(18, self.at(2, 1), 1)

    SHARED = {(0, 0): 3, (-1, 0): 5, (1, 0): 7, (0, 1): 10, (2, 0): 11, (-1, 1): 14, (1, 1): 16, (2, 1): 17}

    def recv_sibling(self, r, p):
        if (r, p) == (2, 1) and not self.far_by_pair:
            self.recv(17, self.at(r, p, 1), 0)
            self.recv(18, self.at(r, p, 1), 1)
        else:
            self.recv(self.SHARED[(r, p)], self.at(r, p, 1))

    def finish(self):
        for i, block, target, half in self.sent:
            self.copy(i, block, target, half).wait_send()


ORDER = ((0, 0), (-1, 0), (1, 0), (0, 1), (2, 0), (-1, 1), (1, 1), (2, 1))


def pick(index, values):
    out = values[0]
    for i, v in enumerate(values[1:], 1):
        out = jnp.where(index == i, v, out)
    return out


def greet(k, peers):
    barrier = pltpu.get_barrier_semaphore()
    for p in peers:
        pl.semaphore_signal(barrier, inc=1, device_id=device(p), device_id_type=MESH)
    pl.semaphore_wait(barrier, len(peers))


def tensor_peers(k):
    return [moved(k, x=r, zh=p) for r, p in ORDER[1:]]


def seq_peers(k):
    return [
        moved(k, y=r, zl=p, c=c) for r, p in ORDER for c in (0, 1) if (r, p, c) != (0, 0, 0)
    ]


def as_columns(rows):
    parts = [jnp.broadcast_to(rows[i : i + 1, :], (128, 128)).T for i in range(rows.shape[0])]
    return jnp.concatenate(parts, 0)


QT = 128
CHUNKS = ((0, 1), (1, 1), (2, 1), (3, 1))
GROUP = 2
ALONG = (64, 0)


def block_kernel(
    tokens, pos, gain_in, w_query, w_key, w_value, b_query, b_key, b_value, freq_in, w_out,
    mixed, context, gain, bias, freq, cosine, sine,
    x_all, w_all, acc, normed, ssq, inverse, wo_mid, pos_all,
    q, kv_all, wo_all, ctx_all, key_pos, own_pos, top, low, num, mixed_v,
    local_sem, x_ssem, x_rsem, w_ssem, w_rsem, s_ssem, s_rsem, p_ssem, p_rsem, t_ssem, t_rsem,
    kv_ssem, kv_rsem, wo_ssem, wo_rsem, c_ssem, c_rsem, out_sem,
):
    k = coords()
    me_s, me_t = seq_of(k), tensor_of(k)
    rows = tokens.shape[0]
    qc, kc = w_query.shape[1], w_key.shape[1]
    wrows = w_query.shape[0]
    heads = qc // HD
    cw = qc

    loads = [
        pltpu.make_async_copy(tokens, x_all.at[me_t], local_sem.at[0]),
        pltpu.make_async_copy(w_query, w_all.at[me_s, :, pl.ds(0, qc)], local_sem.at[1]),
        pltpu.make_async_copy(w_key, w_all.at[me_s, :, pl.ds(qc, kc)], local_sem.at[2]),
        pltpu.make_async_copy(w_value, w_all.at[me_s, :, pl.ds(qc + kc, kc)], local_sem.at[3]),
        pltpu.make_async_copy(pos, pos_all.at[me_s], local_sem.at[4]),
        pltpu.make_async_copy(gain_in, gain, local_sem.at[6]),
        pltpu.make_async_copy(b_query, bias.at[:, pl.ds(0, qc)], local_sem.at[7]),
        pltpu.make_async_copy(b_key, bias.at[:, pl.ds(qc, kc)], local_sem.at[8]),
        pltpu.make_async_copy(b_value, bias.at[:, pl.ds(qc + kc, kc)], local_sem.at[9]),
        pltpu.make_async_copy(freq_in, freq, local_sem.at[10]),
    ]
    for c in loads:
        c.start()
    greet(k, tensor_peers(k) + seq_peers(k))
    for c in loads:
        c.wait()

    def wo_slot(b):
        return wo_all.at[:, seq_of(b) // 2, :, pl.ds(pl.multiple_of(b["c"] * cw, cw), cw)]

    def ctx_slot(first, count):
        return lambda b: ctx_all.at[
            pl.ds(first * QT, count * QT), pl.ds(pl.multiple_of(tensor_of(b) * cw, cw), cw)
        ]

    part_rows = rows // 2
    xg = [
        Gather(
            k, lambda b, h=h: x_all.at[tensor_of(b), pl.ds(h * part_rows, part_rows)], part_rows // 2,
            "x", "zh", False, x_ssem, x_rsem, base=10 * h, along=ALONG[h],
        )
        for h in range(2)
    ]
    wg = Gather(k, lambda b: w_all.at[seq_of(b)], wrows // 2, "y", "zl", True, w_ssem, w_rsem)
    def kv_rows(h, b):
        return pl.ds(pl.multiple_of((h * 16 + seq_of(b)) * part_rows, part_rows), part_rows)

    kg = [
        Gather(
            k, lambda b, h=h: kv_all.at[kv_rows(h, b)], part_rows // 2, "y", "zl", True,
            kv_ssem, kv_rsem, base=18 * h, far_by_pair=h == 1,
        )
        for h in range(2)
    ]
    og = Gather(
        k, wo_slot, wo_all.shape[0] // 2, "y", "zl", True, wo_ssem, wo_rsem
    )
    cg = [
        Gather(k, ctx_slot(f, n), n * QT // 2, "x", "zh", False, c_ssem, c_rsem, base=8 * i)
        for i, (f, n) in enumerate(CHUNKS)
    ]

    eighth = wo_mid.shape[1]

    def spread_copy(i, source, target):
        return pltpu.make_async_remote_copy(
            w_out.at[pl.ds((seq_of(target) // 2) * eighth, eighth)], wo_mid.at[seq_of(source) // 2],
            t_ssem.at[i], t_rsem.at[i], device_id=device(target), device_id_type=MESH,
        )

    def wo_part(t):
        return wo_all.at[t, me_s // 2, :, pl.ds(pl.multiple_of(k["c"] * cw, cw), cw)]

    def settle_copy(i, source, target):
        return pltpu.make_async_remote_copy(
            wo_mid.at[tensor_of(target)], wo_part(tensor_of(source)),
            t_ssem.at[8 + i], t_rsem.at[8 + i], device_id=device(target), device_id_type=MESH,
        )

    spread_own = pltpu.make_async_copy(
        w_out.at[pl.ds((me_s // 2) * eighth, eighth)], wo_mid.at[me_s // 2], t_ssem.at[7]
    )
    settle_own = pltpu.make_async_copy(wo_mid.at[me_t], wo_part(me_t), t_ssem.at[15])

    def pos_copy(i, b, target):
        ref = pos_all.at[seq_of(b)]
        return pltpu.make_async_remote_copy(
            ref, ref, p_ssem.at[i], p_rsem.at[i], device_id=device(target), device_id_type=MESH
        )

    s_list = [(r, p, c) for r, p in ORDER for c in (0, 1) if (r, p, c) != (0, 0, 0)]

    def ssq_copy(i, b, target):
        ref = ssq.at[tensor_of(b)]
        return pltpu.make_async_remote_copy(
            ref, ref, s_ssem.at[i], s_rsem.at[i], device_id=device(target), device_id_type=MESH
        )

    wg.s0()
    xg[0].s0_ring()
    xg[1].s0_ring()
    for i in range(rows // 128):
        xb = x_all[me_t, pl.ds(i * 128, 128), :].astype(F32)
        total = jnp.sum(xb * xb, -1, keepdims=True)
        ssq[me_t, i : i + 1, :] = jnp.broadcast_to(total, (128, 128)).T[0:1, :]
    for i, (r, p, c) in enumerate(s_list):
        pos_copy(i, k, moved(k, y=r, zl=p, c=c)).start()
    acc[...] = jnp.zeros_like(acc)
    top[...] = jnp.full_like(top, NEG_FILL)
    low[...] = jnp.zeros_like(low)
    num[...] = jnp.zeros_like(num)
    for i, (r, p) in enumerate(ORDER[1:]):
        ssq_copy(i, k, moved(k, x=r, zh=p)).start()

    wg.s1()
    wg.s2()
    xg[0].s0_pair()
    xg[0].s1()
    xg[1].s1()
    for i, (r, p) in enumerate(ORDER[1:]):
        ssq_copy(i, moved(k, x=-r, zh=p), k).wait_recv()
    total = ssq[0]
    for i in range(1, 8):
        total = total + ssq[i]
    scale = lax.rsqrt(total / (8 * x_all.shape[2]) + NORM_EPS)
    inverse[...] = as_columns(scale[0 : rows // 128, :])
    wg.s3()
    xg[0].s3()
    xg[1].s0_pair()
    xg[0].s2()
    xg[1].s3()
    wg.s4()
    for i, (r, p) in enumerate(ORDER[1:]):
        spread_copy(i, k, moved(k, y=r, zl=p)).start()
    spread_own.start()
    xg[0].s4()
    xg[1].s2()
    for i, (r, p, c) in enumerate(s_list):
        pos_copy(i, moved(k, y=-r, zl=p, c=c), k).wait_recv()

    def spread(s, carry):
        for h in range(2):
            for j in range(part_rows // 128):
                row = h * (part_rows // 128) + j
                key_pos[h * 16 + s, :, j * 128 : (j + 1) * 128] = pos_all[s, row : row + 1, :].astype(F32)
        return carry

    lax.fori_loop(0, pos_all.shape[0], spread, 0)
    own_pos[...] = as_columns(pos_all[me_s].astype(F32))
    lane = lax.broadcasted_iota(jnp.int32, (128, HD), 1)
    for i in range(rows // 128):
        r = slice(i * 128, (i + 1) * 128)
        angles = own_pos[r, :] * freq[...]
        cosine[r, :] = jnp.cos(angles)
        turn = jnp.sin(angles)
        sine[r, :] = jnp.where(lane < HD // 2, -turn, turn)
    def settle():
        for i, (r, p) in enumerate(ORDER[1:]):
            spread_copy(i, moved(k, y=-r, zl=p), moved(k, y=r, zl=p)).wait_recv()
        spread_own.wait()
        for i, (r, p) in enumerate(ORDER[1:]):
            settle_copy(i, k, moved(k, x=r, zh=p)).start()
        settle_own.start()

    def settled():
        for i, (r, p) in enumerate(ORDER[1:]):
            settle_copy(i, moved(k, x=-r, zh=p), moved(k, x=r, zh=p)).wait_recv()
        settle_own.wait()

    wg.s5()
    for r, p in ORDER:
        wg.recv_sibling(r, p)

    cos_sin = (cosine, sine)

    def project(h):
        first = h * part_rows

        def block(step, carry):
            if h == 1:

                @pl.when(step == 5)
                def _():
                    xg[1].s4()

                @pl.when(step == 7)
                def _():
                    kg[0].s1()
                    kg[0].s2()
                    xg[1].s5()
                    settle()

            dx = pick(step, [r % 4 for r, _ in ORDER])
            dz = pick(step, [p for _, p in ORDER])
            t = ((k["zh"] + dz) % 2) * 4 + (k["x"] + dx) % 4
            g = gain[t]
            for i in range(part_rows // 128):
                r = pl.ds(first + i * 128, 128)
                inv = inverse[r, :]
                for j in range(x_all.shape[2] // 128):
                    piece = x_all[t, r, pl.ds(j * 128, 128)].astype(F32)
                    normed[pl.ds(i * 128, 128), pl.ds(j * 128, 128)] = (
                        piece * inv * g[:, j * 128 : (j + 1) * 128]
                    ).astype(BF16)
            part = jnp.dot(normed[:, 0:wrows], w_all[2 * t], preferred_element_type=F32)
            part = part + jnp.dot(
                normed[:, wrows : 2 * wrows], w_all[2 * t + 1], preferred_element_type=F32
            )
            acc[first : first + part_rows, :] += part
            return carry

        lax.fori_loop(0, 8, block, 0)
        r = slice(first, first + part_rows)
        cos, sin = (x[r, :] for x in cos_sin)

        def turned(head):
            u = acc[r, head * HD : (head + 1) * HD] + bias[:, head * HD : (head + 1) * HD]
            return (u * cos + pltpu.roll(u, HD // 2, 1) * sin).astype(BF16)

        own = kv_rows(h, k)
        kv_all[own, 0:HD] = turned(heads)
        kv_all[own, HD : 2 * HD] = (acc[r, qc + kc :] + bias[:, qc + kc :]).astype(BF16)
        for head in range(heads):
            q[head, r, :] = turned(head)

    xg[0].s5()
    project(0)
    kg[0].s0()
    project(1)
    kg[1].s0()

    factor = HD ** (-0.5) / math.log(2.0)
    keys = 2 * rows
    tiles = rows // QT
    events = {}

    def event(step, *fns):
        events.setdefault(step, []).extend(fns)

    def sib(h, r):
        return lambda: (kg[h].recv_sibling(r, 0), kg[h].recv_sibling(r, 1))

    def close(i):
        f, n = CHUNKS[i]
        r = pl.ds(f * QT, n * QT)
        for h in range(heads):
            bottom = jnp.sum(low[h, r, :], -1, keepdims=True)
            done = (num[h, r, :] / bottom).astype(BF16)
            ctx_all[r, pl.ds(pl.multiple_of(me_t * cw + h * HD, HD), HD)] = done

    def send_ctx(i):
        cg[i].s0()

    def settle_sends():
        for i, (r, p) in enumerate(ORDER[1:]):
            spread_copy(i, k, moved(k, y=r, zl=p)).wait_send()
            settle_copy(i, k, moved(k, x=r, zh=p)).wait_send()
            ssq_copy(i, k, moved(k, x=r, zh=p)).wait_send()
        for i, (r, p, c) in enumerate(s_list):
            pos_copy(i, k, moved(k, y=r, zl=p, c=c)).wait_send()
        for x in [*xg, wg]:
            x.finish()

    def ctx_last(i):
        cg[i].s4()
        cg[i].s5()

    event(0, sib(0, 0))
    event(2, kg[0].s3, kg[0].s4, sib(0, -1))
    event(3, kg[1].s1, kg[1].s2, settled, og.s0_ring, sib(0, 1))
    event(4, kg[1].s3, og.s0_pair, sib(1, 0), kg[0].s5)
    event(5, sib(0, 2))
    event(6, kg[1].s4, sib(1, -1))
    event(7, sib(1, 1), settle_sends)
    event(8, kg[1].s5, sib(1, 2))
    event(9, lambda: close(0), lambda: send_ctx(0), lambda: close(1), lambda: send_ctx(1))
    event(10, og.s1)
    event(12, cg[0].s1, og.s2, cg[0].s2)
    event(13, lambda: close(2), lambda: send_ctx(2), cg[1].s1)
    event(14, cg[0].s3)

    def dispatch(g, first, last):
        if last - first == 1:
            for fn in events.get(first, []):
                fn()
            return
        middle = (first + last) // 2
        lax.cond(
            g < middle, lambda: dispatch(g, first, middle), lambda: dispatch(g, middle, last)
        )

    def step(g, carry):
        dispatch(g, 0, 4 * tiles)
        units = [Unit(2 * g + half, u) for half in range(2) for u in range(heads // GROUP)]
        s, held = units[0].scores(), None
        for i, unit in enumerate(units):
            later = units[i + 1].scores() if i + 1 < len(units) else None
            now = unit.soften(s)
            if held is not None:
                units[i - 1].collect(*held)
            s, held = later, now
        units[-1].collect(*held)
        return carry

    class Unit:
        def __init__(self, g, u):
            late = jnp.maximum(g - 18, 0)
            mid = jnp.maximum(g - 4, 0)
            kb = jnp.where(g < 4, 0, jnp.where(g < 18, 1 + mid // 2, 1 + late % 7))
            tile = jnp.where(g < 4, g, jnp.where(g < 18, mid % 2, 2 + late // 7))
            dy = pick(kb, [r % 4 for r, _ in ORDER])
            dz = pick(kb, [p for _, p in ORDER])
            self.block = dz * 4 + (k["y"] + dy) % 4
            self.kr = pl.ds(pl.multiple_of(self.block * keys, keys), keys)
            self.at = (slice(u * GROUP, (u + 1) * GROUP), pl.ds(pl.multiple_of(tile * QT, QT), QT), slice(None))
            self.mine = jnp.concatenate([own_pos[self.at[1], :]] * GROUP, 0)

        def scores(self):
            return lax.dot_general(
                q[self.at].reshape(GROUP * QT, HD), kv_all[self.kr, 0:HD], (((1,), (1,)), ((), ())),
                preferred_element_type=F32,
            )

        def soften(self, s):
            parts = []
            for j in range(keys // 128):
                lane = (j % (part_rows // 128)) * 128
                kp = key_pos[self.block * 4 + j // (part_rows // 128), :, lane : lane + 128]
                parts.append(jnp.where(kp <= self.mine, s[:, j * 128 : (j + 1) * 128], NEG_FILL))
            best = parts[0]
            for x in parts[1:]:
                best = jnp.maximum(best, x)
            old = top[self.at].reshape(GROUP * QT, 128)
            new = jnp.maximum(old, jnp.max(best, -1, keepdims=True))
            top[self.at] = new.reshape(GROUP, QT, 128)
            alpha = jnp.exp2((old - new) * factor)
            weights, total = [], low[self.at].reshape(GROUP * QT, 128) * alpha
            for x in parts:
                w = jnp.exp2((x - new) * factor)
                total = total + w
                weights.append(w.astype(BF16))
            low[self.at] = total.reshape(GROUP, QT, 128)
            return alpha, jnp.concatenate(weights, 1)

        def collect(self, alpha, weights):
            out = num[self.at].reshape(GROUP * QT, HD) * alpha + jnp.dot(
                weights, kv_all[self.kr, HD : 2 * HD], preferred_element_type=F32
            )
            num[self.at] = out.reshape(GROUP, QT, HD)

    lax.fori_loop(0, 4 * tiles, step, 0)

    close(3)
    send_ctx(3)
    cg[2].s1()
    cg[1].s2()
    def output(first, count):
        r = pl.ds(first * QT, count * QT)

        def put_part(c):
            cols = pl.ds(pl.multiple_of(c * 256, 256), 256)
            return pltpu.make_async_copy(mixed_v.at[r, cols], mixed.at[r, cols], out_sem.at[0, c])

        def part(c, carry):
            cols = pl.ds(pl.multiple_of(c * 256, 256), 256)
            w = wo_all[:, :, :, cols].reshape(ctx_all.shape[1], 256)
            summed = jnp.dot(ctx_all[r, :], w, preferred_element_type=F32)
            mixed_v[r, cols] = (x_all[me_t, r, cols].astype(F32) + summed).astype(BF16)
            put_part(c).start()
            return carry

        lax.fori_loop(0, mixed.shape[1] // 256, part, 0)
        return [put_part(c) for c in range(mixed.shape[1] // 256)]

    put = pltpu.make_async_copy(
        ctx_all.at[:, pl.ds(pl.multiple_of(me_t * cw, cw), cw)], context, local_sem.at[5]
    )
    put.start()
    kg[0].finish()
    kg[1].finish()
    cg[1].s3()
    og.s3()
    cg[0].s4()
    cg[3].s1()
    og.s4()
    cg[2].s2()
    cg[3].s2()
    cg[2].s3()
    cg[3].s3()
    cg[0].s5()
    ctx_last(1)
    og.s5()
    for r, p in ORDER:
        og.recv_sibling(r, p)
    ctx_last(2)
    ctx_last(3)
    puts = [put, *output(0, 4)]
    for x in [og, *cg]:
        x.finish()
    for c in puts:
        c.wait()


def shards(tokens, positions, norm_gain, w_query, w_key, w_value, b_query, b_key, b_value, w_out):
    rows, feats = tokens.shape
    qc, kc = w_query.shape[1], w_key.shape[1]
    wrows = w_query.shape[0]
    heads = qc // HD
    nt, ns = lax.axis_size("tensor"), lax.axis_size("seq")
    inv_freq = ROPE_BASE ** (-np.arange(HD // 2, dtype=np.float64) * 2.0 / HD)
    freq = jnp.asarray(np.concatenate([inv_freq, inv_freq])[None, :].astype(np.float32))
    hbm = pl.BlockSpec(memory_space=pltpu.HBM)
    dma = pltpu.SemaphoreType.DMA
    return pl.pallas_call(
        block_kernel,
        name="block",
        out_shape=(
            jax.ShapeDtypeStruct((rows, feats), BF16),
            jax.ShapeDtypeStruct((rows, qc), BF16),
        ),
        in_specs=[hbm] * 11,
        out_specs=(pl.BlockSpec(memory_space=pl.ANY), pl.BlockSpec(memory_space=pl.ANY)),
        scratch_shapes=[
            pltpu.VMEM((nt, 1, feats), F32),
            pltpu.VMEM((1, qc + 2 * kc), F32),
            pltpu.VMEM((1, HD), F32),
            pltpu.VMEM((rows, HD), F32),
            pltpu.VMEM((rows, HD), F32),
            pltpu.VMEM((nt, rows, feats), BF16),
            pltpu.VMEM((ns, wrows, qc + 2 * kc), BF16),
            pltpu.VMEM((rows, qc + 2 * kc), F32),
            pltpu.VMEM((rows // 2, feats), BF16),
            pltpu.VMEM((nt, 8, 128), F32),
            pltpu.VMEM((rows, 128), F32),
            pltpu.VMEM((nt, w_out.shape[0] // 8, w_out.shape[1]), BF16),
            pltpu.VMEM((ns, rows // 128, 128), jnp.int32),
            pltpu.VMEM((heads, rows, HD), BF16),
            pltpu.VMEM((ns * rows, 2 * HD), BF16),
            pltpu.VMEM((nt, 8, qc // 8, feats), BF16),
            pltpu.VMEM((rows, nt * qc), BF16),
            pltpu.VMEM((2 * ns, 1, rows // 2), F32),
            pltpu.VMEM((rows, 128), F32),
            pltpu.VMEM((heads, rows, 128), F32),
            pltpu.VMEM((heads, rows, 128), F32),
            pltpu.VMEM((heads, rows, HD), F32),
            pltpu.VMEM((rows, feats), BF16),
            dma((12,)), dma((20,)), dma((20,)), dma((18,)), dma((18,)),
            dma((7,)), dma((7,)), dma((15,)), dma((15,)), dma((16,)), dma((15,)),
            dma((36,)), dma((36,)), dma((18,)), dma((18,)), dma((32,)), dma((32,)), dma((1, 4)),
        ],
        compiler_params=pltpu.CompilerParams(
            collective_id=0, has_side_effects=True, vmem_limit_bytes=58 * 1024 * 1024
        ),
    )(
        tokens, positions.reshape(rows // 128, 128), norm_gain.reshape(nt, 1, feats), w_query, w_key, w_value,
        b_query[None, :], b_key[None, :], b_value[None, :], freq, w_out,
    )


def solution(mesh):
    in_specs = (
        P("seq", "tensor"),
        P("seq"),
        P(),
        P("seq", "tensor"),
        P("seq", "tensor"),
        P("seq", "tensor"),
        P("tensor"),
        P("tensor"),
        P("tensor"),
        P("tensor", "seq"),
    )
    out_specs = (P("seq", "tensor"), P("seq", "tensor"))
    return jax.shard_map(shards, mesh=mesh, in_specs=in_specs, out_specs=out_specs, check_vma=False)
```

```python
import functools
import math

import jax
import jax.numpy as jnp
import numpy as np
from jax import lax
from jax.experimental import pallas as pl
from jax.experimental.pallas import tpu as pltpu
from jax.sharding import PartitionSpec as P

HD = 128
NORM_EPS = 1e-06
ROPE_BASE = 1000000.0
NEG_FILL = -1e30
MESH = pl.DeviceIdType.MESH
BF16 = jnp.bfloat16
F32 = jnp.float32


def coords():
    s, t = lax.axis_index("seq"), lax.axis_index("tensor")
    return dict(y=s // 4, zl=(s // 2) % 2, c=s % 2, zh=t // 4, x=t % 4)


SIZES = dict(y=4, zl=2, c=2, zh=2, x=4)


def moved(k, **shift):
    k = dict(k)
    for name, by in shift.items():
        k[name] = (k[name] + (by + SIZES[name])) % SIZES[name]
    return k


def seq_of(k):
    return k["y"] * 4 + k["zl"] * 2 + k["c"]


def tensor_of(k):
    return k["zh"] * 4 + k["x"]


def device(k):
    return (seq_of(k), tensor_of(k))


SHARING = (0, 1, 2, 3, 4, 5, 6, 7, 8, 9, 10, 11, 13, 14, 15, 16, 17, 18)
ALONE = (0, 1, 2, 4, 6, 8, 9, 13, 14, 15)


class Gather:
    def __init__(self, k, slot, half_rows, ring, pair, sibling, ssem, rsem, base=0, along=0, far_by_pair=False):
        self.k, self.slot, self.half = k, slot, half_rows
        self.ring, self.pair, self.sibling = ring, pair, sibling
        self.ssem, self.rsem, self.base = ssem, rsem, base
        self.along, self.direct = along, 2 * half_rows - 2 * along
        self.far_by_pair = far_by_pair or not sibling
        self.used = SHARING if sibling else ALONE
        self.sent = []

    def at(self, r=0, p=0, c=0):
        return (r, p, c)

    def place(self, where):
        r, p, c = where
        return moved(self.k, **{self.ring: r, self.pair: p, "c": c})

    def copy(self, i, block, target, half):
        ref = self.slot(self.place(block))
        if half is not None:
            first, count = half if isinstance(half, tuple) else (half * self.half, self.half)
            ref = ref.at[pl.ds(first, count)]
        return pltpu.make_async_remote_copy(
            src_ref=ref,
            dst_ref=ref,
            send_sem=self.ssem.at[self.base + self.used.index(i)],
            recv_sem=self.rsem.at[self.base + self.used.index(i)],
            device_id=device(self.place(target)),
            device_id_type=MESH,
        )

    def send(self, i, block, target, half=None):
        self.copy(i, block, target, half).start()
        self.sent.append((i, block, target, half))

    def recv(self, i, block, half=None):
        self.copy(i, block, (0, 0, 1) if self.sibling else (1, 0, 0), half).wait_recv()

    def share(self, i, block, half=None):
        if self.sibling:
            self.send(i, block, self.at(c=1), half)

    def s0(self):
        self.s0_ring()
        self.s0_pair()

    def s0_ring(self):
        self.send(0, self.at(), self.at(1))
        self.send(1, self.at(), self.at(-1))
        self.share(3, self.at())

    def s0_pair(self):
        self.send(2, self.at(), self.at(p=1))

    def s1(self):
        self.recv(0, self.at(-1))
        self.send(4, self.at(-1), self.at(1), 0)
        self.share(5, self.at(-1))
        self.recv(1, self.at(1))
        self.send(6, self.at(1), self.at(-1), 1)
        self.share(7, self.at(1))

    def s2(self):
        self.recv(2, self.at(p=1))
        self.send(8, self.at(p=1), self.at(1))
        self.send(9, self.at(p=1), self.at(-1))
        self.share(10, self.at(p=1))

    def s3(self):
        self.recv(4, self.at(2), 0)
        self.recv(6, self.at(2), 1)
        self.share(11, self.at(2))
        if self.far_by_pair:
            self.send(13, self.at(2), self.at(p=1), (0, self.direct))

    def s4(self):
        self.recv(8, self.at(-1, 1))
        if not self.far_by_pair:
            self.send(13, self.at(-1, 1), self.at(1), 0)
        elif self.along:
            self.send(14, self.at(-1, 1), self.at(1), (self.direct, self.along))
        self.share(14, self.at(-1, 1))
        self.recv(9, self.at(1, 1))
        if not self.far_by_pair:
            self.send(15, self.at(1, 1), self.at(-1), 1)
        elif self.along:
            self.send(15, self.at(1, 1), self.at(-1), (self.direct + self.along, self.along))
        self.share(16, self.at(1, 1))

    def s5(self):
        if self.far_by_pair:
            self.recv(13, self.at(2, 1), (0, self.direct))
            if self.along:
                self.recv(14, self.at(2, 1), (self.direct, self.along))
                self.recv(15, self.at(2, 1), (self.direct + self.along, self.along))
            self.share(17, self.at(2, 1))
        else:
            self.recv(13, self.at(2, 1), 0)
            self.share(17, self.at(2, 1), 0)
            self.recv(15, self.at(2, 1), 1)
            self.share(18, self.at(2, 1), 1)

    SHARED = {(0, 0): 3, (-1, 0): 5, (1, 0): 7, (0, 1): 10, (2, 0): 11, (-1, 1): 14, (1, 1): 16, (2, 1): 17}

    def recv_sibling(self, r, p):
        if (r, p) == (2, 1) and not self.far_by_pair:
            self.recv(17, self.at(r, p, 1), 0)
            self.recv(18, self.at(r, p, 1), 1)
        else:
            self.recv(self.SHARED[(r, p)], self.at(r, p, 1))

    def finish(self):
        for i, block, target, half in self.sent:
            self.copy(i, block, target, half).wait_send()


ORDER = ((0, 0), (-1, 0), (1, 0), (0, 1), (2, 0), (-1, 1), (1, 1), (2, 1))


def pick(index, values):
    out = values[0]
    for i, v in enumerate(values[1:], 1):
        out = jnp.where(index == i, v, out)
    return out


def greet(k, peers):
    barrier = pltpu.get_barrier_semaphore()
    for p in peers:
        pl.semaphore_signal(barrier, inc=1, device_id=device(p), device_id_type=MESH)
    pl.semaphore_wait(barrier, len(peers))


def tensor_peers(k):
    return [moved(k, x=r, zh=p) for r, p in ORDER[1:]]


def seq_peers(k):
    return [
        moved(k, y=r, zl=p, c=c) for r, p in ORDER for c in (0, 1) if (r, p, c) != (0, 0, 0)
    ]


def as_columns(rows):
    parts = [jnp.broadcast_to(rows[i : i + 1, :], (128, 128)).T for i in range(rows.shape[0])]
    return jnp.concatenate(parts, 0)


QT = 128
CHUNKS = ((0, 1), (1, 1), (2, 1), (3, 1))
GROUP = 2
ALONG = (64, 0)


def block_kernel(
    tokens, pos, gain_in, w_query, w_key, w_value, b_query, b_key, b_value, freq_in, w_out,
    mixed, context, gain, bias, freq, cosine, sine,
    x_all, w_all, acc, normed, ssq, inverse, wo_mid, pos_all,
    q, kv_all, wo_all, ctx_all, key_pos, own_pos, top, low, num, mixed_v,
    local_sem, x_ssem, x_rsem, w_ssem, w_rsem, s_ssem, s_rsem, p_ssem, p_rsem, t_ssem, t_rsem,
    kv_ssem, kv_rsem, wo_ssem, wo_rsem, c_ssem, c_rsem, out_sem,
):
    k = coords()
    me_s, me_t = seq_of(k), tensor_of(k)
    rows = tokens.shape[0]
    qc, kc = w_query.shape[1], w_key.shape[1]
    wrows = w_query.shape[0]
    heads = qc // HD
    cw = qc

    loads = [
        pltpu.make_async_copy(tokens, x_all.at[me_t], local_sem.at[0]),
        pltpu.make_async_copy(w_query, w_all.at[me_s, :, pl.ds(0, qc)], local_sem.at[1]),
        pltpu.make_async_copy(w_key, w_all.at[me_s, :, pl.ds(qc, kc)], local_sem.at[2]),
        pltpu.make_async_copy(w_value, w_all.at[me_s, :, pl.ds(qc + kc, kc)], local_sem.at[3]),
        pltpu.make_async_copy(pos, pos_all.at[me_s], local_sem.at[4]),
        pltpu.make_async_copy(gain_in, gain, local_sem.at[6]),
        pltpu.make_async_copy(b_query, bias.at[:, pl.ds(0, qc)], local_sem.at[7]),
        pltpu.make_async_copy(b_key, bias.at[:, pl.ds(qc, kc)], local_sem.at[8]),
        pltpu.make_async_copy(b_value, bias.at[:, pl.ds(qc + kc, kc)], local_sem.at[9]),
        pltpu.make_async_copy(freq_in, freq, local_sem.at[10]),
    ]
    for c in loads:
        c.start()
    greet(k, tensor_peers(k) + seq_peers(k))
    for c in loads:
        c.wait()

    def wo_slot(b):
        return wo_all.at[:, seq_of(b) // 2, :, pl.ds(pl.multiple_of(b["c"] * cw, cw), cw)]

    def ctx_slot(first, count):
        return lambda b: ctx_all.at[
            pl.ds(first * QT, count * QT), pl.ds(pl.multiple_of(tensor_of(b) * cw, cw), cw)
        ]

    part_rows = rows // 2
    xg = [
        Gather(
            k, lambda b, h=h: x_all.at[tensor_of(b), pl.ds(h * part_rows, part_rows)], part_rows // 2,
            "x", "zh", False, x_ssem, x_rsem, base=10 * h, along=ALONG[h],
        )
        for h in range(2)
    ]
    wg = Gather(k, lambda b: w_all.at[seq_of(b)], wrows // 2, "y", "zl", True, w_ssem, w_rsem)
    def kv_rows(h, b):
        return pl.ds(pl.multiple_of((h * 16 + seq_of(b)) * part_rows, part_rows), part_rows)

    kg = [
        Gather(
            k, lambda b, h=h: kv_all.at[kv_rows(h, b)], part_rows // 2, "y", "zl", True,
            kv_ssem, kv_rsem, base=18 * h, far_by_pair=h == 1,
        )
        for h in range(2)
    ]
    og = Gather(
        k, wo_slot, wo_all.shape[0] // 2, "y", "zl", True, wo_ssem, wo_rsem
    )
    cg = [
        Gather(k, ctx_slot(f, n), n * QT // 2, "x", "zh", False, c_ssem, c_rsem, base=8 * i)
        for i, (f, n) in enumerate(CHUNKS)
    ]

    eighth = wo_mid.shape[1]

    def spread_copy(i, source, target):
        return pltpu.make_async_remote_copy(
            w_out.at[pl.ds((seq_of(target) // 2) * eighth, eighth)], wo_mid.at[seq_of(source) // 2],
            t_ssem.at[i], t_rsem.at[i], device_id=device(target), device_id_type=MESH,
        )

    def wo_part(t):
        return wo_all.at[t, me_s // 2, :, pl.ds(pl.multiple_of(k["c"] * cw, cw), cw)]

    def settle_copy(i, source, target):
        return pltpu.make_async_remote_copy(
            wo_mid.at[tensor_of(target)], wo_part(tensor_of(source)),
            t_ssem.at[8 + i], t_rsem.at[8 + i], device_id=device(target), device_id_type=MESH,
        )

    spread_own = pltpu.make_async_copy(
        w_out.at[pl.ds((me_s // 2) * eighth, eighth)], wo_mid.at[me_s // 2], t_ssem.at[7]
    )
    settle_own = pltpu.make_async_copy(wo_mid.at[me_t], wo_part(me_t), t_ssem.at[15])

    def pos_copy(i, b, target):
        ref = pos_all.at[seq_of(b)]
        return pltpu.make_async_remote_copy(
            ref, ref, p_ssem.at[i], p_rsem.at[i], device_id=device(target), device_id_type=MESH
        )

    s_list = [(r, p, c) for r, p in ORDER for c in (0, 1) if (r, p, c) != (0, 0, 0)]

    def ssq_copy(i, b, target):
        ref = ssq.at[tensor_of(b)]
        return pltpu.make_async_remote_copy(
            ref, ref, s_ssem.at[i], s_rsem.at[i], device_id=device(target), device_id_type=MESH
        )

    wg.s0()
    xg[0].s0_ring()
    xg[1].s0_ring()
    for i in range(rows // 128):
        xb = x_all[me_t, pl.ds(i * 128, 128), :].astype(F32)
        total = jnp.sum(xb * xb, -1, keepdims=True)
        ssq[me_t, i : i + 1, :] = jnp.broadcast_to(total, (128, 128)).T[0:1, :]
    for i, (r, p, c) in enumerate(s_list):
        pos_copy(i, k, moved(k, y=r, zl=p, c=c)).start()
    acc[...] = jnp.zeros_like(acc)
    top[...] = jnp.full_like(top, NEG_FILL)
    low[...] = jnp.zeros_like(low)
    num[...] = jnp.zeros_like(num)
    for i, (r, p) in enumerate(ORDER[1:]):
        ssq_copy(i, k, moved(k, x=r, zh=p)).start()

    wg.s1()
    wg.s2()
    xg[0].s0_pair()
    xg[0].s1()
    xg[1].s1()
    for i, (r, p) in enumerate(ORDER[1:]):
        ssq_copy(i, moved(k, x=-r, zh=p), k).wait_recv()
    total = ssq[0]
    for i in range(1, 8):
        total = total + ssq[i]
    scale = lax.rsqrt(total / (8 * x_all.shape[2]) + NORM_EPS)
    inverse[...] = as_columns(scale[0 : rows // 128, :])
    wg.s3()
    xg[0].s3()
    xg[1].s0_pair()
    xg[0].s2()
    xg[1].s3()
    wg.s4()
    for i, (r, p) in enumerate(ORDER[1:]):
        spread_copy(i, k, moved(k, y=r, zl=p)).start()
    spread_own.start()
    xg[0].s4()
    xg[1].s2()
    for i, (r, p, c) in enumerate(s_list):
        pos_copy(i, moved(k, y=-r, zl=p, c=c), k).wait_recv()

    def spread(s, carry):
        for h in range(2):
            for j in range(part_rows // 128):
                row = h * (part_rows // 128) + j
                key_pos[h * 16 + s, :, j * 128 : (j + 1) * 128] = pos_all[s, row : row + 1, :].astype(F32)
        return carry

    lax.fori_loop(0, pos_all.shape[0], spread, 0)
    own_pos[...] = as_columns(pos_all[me_s].astype(F32))
    lane = lax.broadcasted_iota(jnp.int32, (128, HD), 1)
    for i in range(rows // 128):
        r = slice(i * 128, (i + 1) * 128)
        angles = own_pos[r, :] * freq[...]
        cosine[r, :] = jnp.cos(angles)
        turn = jnp.sin(angles)
        sine[r, :] = jnp.where(lane < HD // 2, -turn, turn)
    def settle():
        for i, (r, p) in enumerate(ORDER[1:]):
            spread_copy(i, moved(k, y=-r, zl=p), moved(k, y=r, zl=p)).wait_recv()
        spread_own.wait()
        for i, (r, p) in enumerate(ORDER[1:]):
            settle_copy(i, k, moved(k, x=r, zh=p)).start()
        settle_own.start()

    def settled():
        for i, (r, p) in enumerate(ORDER[1:]):
            settle_copy(i, moved(k, x=-r, zh=p), moved(k, x=r, zh=p)).wait_recv()
        settle_own.wait()

    wg.s5()
    for r, p in ORDER[:-1]:
        wg.recv_sibling(r, p)

    cos_sin = (cosine, sine)

    def project(h):
        first = h * part_rows

        def block(step, carry):
            if h == 0:

                @pl.when(step == 7)
                def _():
                    wg.recv_sibling(2, 1)

            if h == 1:

                @pl.when(step == 5)
                def _():
                    xg[1].s4()

                @pl.when(step == 7)
                def _():
                    kg[0].s1()
                    kg[0].s2()
                    xg[1].s5()
                    settle()

            dx = pick(step, [r % 4 for r, _ in ORDER])
            dz = pick(step, [p for _, p in ORDER])
            if h == 0:
                t = ((k["y"] + dx) % 4) * 2 + (k["zl"] + dz) % 2
            else:
                t = ((k["zh"] + dz) % 2) * 4 + (k["x"] + dx) % 4
            g = gain[t]
            for i in range(part_rows // 128):
                r = pl.ds(first + i * 128, 128)
                inv = inverse[r, :]
                for j in range(x_all.shape[2] // 128):
                    piece = x_all[t, r, pl.ds(j * 128, 128)].astype(F32)
                    normed[pl.ds(i * 128, 128), pl.ds(j * 128, 128)] = (
                        piece * inv * g[:, j * 128 : (j + 1) * 128]
                    ).astype(BF16)
            part = jnp.dot(normed[:, 0:wrows], w_all[2 * t], preferred_element_type=F32)
            part = part + jnp.dot(
                normed[:, wrows : 2 * wrows], w_all[2 * t + 1], preferred_element_type=F32
            )
            acc[first : first + part_rows, :] += part
            return carry

        lax.fori_loop(0, 8, block, 0)
        r = slice(first, first + part_rows)
        cos, sin = (x[r, :] for x in cos_sin)

        def turned(head):
            u = acc[r, head * HD : (head + 1) * HD] + bias[:, head * HD : (head + 1) * HD]
            return (u * cos + pltpu.roll(u, HD // 2, 1) * sin).astype(BF16)

        own = kv_rows(h, k)
        kv_all[own, 0:HD] = turned(heads)
        kv_all[own, HD : 2 * HD] = (acc[r, qc + kc :] + bias[:, qc + kc :]).astype(BF16)
        for head in range(heads):
            q[head, r, :] = turned(head)

    xg[0].s5()
    project(0)
    kg[0].s0()
    project(1)
    kg[1].s0()

    factor = HD ** (-0.5) / math.log(2.0)
    keys = 2 * rows
    tiles = rows // QT
    events = {}

    def event(step, *fns):
        events.setdefault(step, []).extend(fns)

    def sib(h, r):
        return lambda: (kg[h].recv_sibling(r, 0), kg[h].recv_sibling(r, 1))

    def close(i):
        f, n = CHUNKS[i]
        r = pl.ds(f * QT, n * QT)
        for h in range(heads):
            bottom = jnp.sum(low[h, r, :], -1, keepdims=True)
            done = (num[h, r, :] / bottom).astype(BF16)
            ctx_all[r, pl.ds(pl.multiple_of(me_t * cw + h * HD, HD), HD)] = done

    def send_ctx(i):
        cg[i].s0()

    def settle_sends():
        for i, (r, p) in enumerate(ORDER[1:]):
            spread_copy(i, k, moved(k, y=r, zl=p)).wait_send()
            settle_copy(i, k, moved(k, x=r, zh=p)).wait_send()
            ssq_copy(i, k, moved(k, x=r, zh=p)).wait_send()
        for i, (r, p, c) in enumerate(s_list):
            pos_copy(i, k, moved(k, y=r, zl=p, c=c)).wait_send()
        for x in [*xg, wg]:
            x.finish()

    def ctx_last(i):
        cg[i].s4()
        cg[i].s5()

    event(0, sib(0, 0))
    event(2, kg[0].s3, kg[0].s4, sib(0, -1))
    event(3, kg[1].s1, kg[1].s2, settled, og.s0_ring, sib(0, 1))
    event(4, kg[1].s3, og.s0_pair, sib(1, 0), kg[0].s5)
    event(5, sib(0, 2))
    event(6, kg[1].s4, sib(1, -1))
    event(7, sib(1, 1), settle_sends)
    event(8, kg[1].s5, sib(1, 2))
    event(9, lambda: close(0), lambda: send_ctx(0), lambda: close(1), lambda: send_ctx(1))
    event(10, og.s1)
    event(12, cg[0].s1, og.s2, cg[0].s2)
    event(13, lambda: close(2), lambda: send_ctx(2), cg[1].s1)
    event(14, cg[0].s3)

    def dispatch(g, first, last):
        if last - first == 1:
            for fn in events.get(first, []):
                fn()
            return
        middle = (first + last) // 2
        lax.cond(
            g < middle, lambda: dispatch(g, first, middle), lambda: dispatch(g, middle, last)
        )

    def step(g, carry):
        dispatch(g, 0, 4 * tiles)
        units = [Unit(2 * g + half, u) for half in range(2) for u in range(heads // GROUP)]
        s, held = units[0].scores(), None
        for i, unit in enumerate(units):
            later = units[i + 1].scores() if i + 1 < len(units) else None
            now = unit.soften(s)
            if held is not None:
                units[i - 1].collect(*held)
            s, held = later, now
        units[-1].collect(*held)
        return carry

    class Unit:
        def __init__(self, g, u):
            late = jnp.maximum(g - 18, 0)
            mid = jnp.maximum(g - 4, 0)
            kb = jnp.where(g < 4, 0, jnp.where(g < 18, 1 + mid // 2, 1 + late % 7))
            tile = jnp.where(g < 4, g, jnp.where(g < 18, mid % 2, 2 + late // 7))
            dy = pick(kb, [r % 4 for r, _ in ORDER])
            dz = pick(kb, [p for _, p in ORDER])
            self.block = dz * 4 + (k["y"] + dy) % 4
            self.kr = pl.ds(pl.multiple_of(self.block * keys, keys), keys)
            self.at = (slice(u * GROUP, (u + 1) * GROUP), pl.ds(pl.multiple_of(tile * QT, QT), QT), slice(None))
            self.mine = jnp.concatenate([own_pos[self.at[1], :]] * GROUP, 0)

        def scores(self):
            return lax.dot_general(
                q[self.at].reshape(GROUP * QT, HD), kv_all[self.kr, 0:HD], (((1,), (1,)), ((), ())),
                preferred_element_type=F32,
            )

        def soften(self, s):
            parts = []
            for j in range(keys // 128):
                lane = (j % (part_rows // 128)) * 128
                kp = key_pos[self.block * 4 + j // (part_rows // 128), :, lane : lane + 128]
                parts.append(jnp.where(kp <= self.mine, s[:, j * 128 : (j + 1) * 128], NEG_FILL))
            best = parts[0]
            for x in parts[1:]:
                best = jnp.maximum(best, x)
            old = top[self.at].reshape(GROUP * QT, 128)
            new = jnp.maximum(old, jnp.max(best, -1, keepdims=True))
            top[self.at] = new.reshape(GROUP, QT, 128)
            alpha = jnp.exp2((old - new) * factor)
            weights, total = [], low[self.at].reshape(GROUP * QT, 128) * alpha
            for x in parts:
                w = jnp.exp2((x - new) * factor)
                total = total + w
                weights.append(w.astype(BF16))
            low[self.at] = total.reshape(GROUP, QT, 128)
            return alpha, jnp.concatenate(weights, 1)

        def collect(self, alpha, weights):
            out = num[self.at].reshape(GROUP * QT, HD) * alpha + jnp.dot(
                weights, kv_all[self.kr, HD : 2 * HD], preferred_element_type=F32
            )
            num[self.at] = out.reshape(GROUP, QT, HD)

    lax.fori_loop(0, 4 * tiles, step, 0)

    close(3)
    send_ctx(3)
    cg[2].s1()
    cg[1].s2()
    def output(first, count):
        r = pl.ds(first * QT, count * QT)

        def put_part(c):
            cols = pl.ds(pl.multiple_of(c * 256, 256), 256)
            return pltpu.make_async_copy(mixed_v.at[r, cols], mixed.at[r, cols], out_sem.at[0, c])

        def part(c, carry):
            cols = pl.ds(pl.multiple_of(c * 256, 256), 256)
            w = wo_all[:, :, :, cols].reshape(ctx_all.shape[1], 256)
            summed = jnp.dot(ctx_all[r, :], w, preferred_element_type=F32)
            mixed_v[r, cols] = (x_all[me_t, r, cols].astype(F32) + summed).astype(BF16)
            put_part(c).start()
            return carry

        lax.fori_loop(0, mixed.shape[1] // 256, part, 0)
        return [put_part(c) for c in range(mixed.shape[1] // 256)]

    put = pltpu.make_async_copy(
        ctx_all.at[:, pl.ds(pl.multiple_of(me_t * cw, cw), cw)], context, local_sem.at[5]
    )
    put.start()
    kg[0].finish()
    kg[1].finish()
    cg[1].s3()
    og.s3()
    cg[0].s4()
    cg[3].s1()
    og.s4()
    cg[2].s2()
    cg[3].s2()
    cg[2].s3()
    cg[3].s3()
    cg[0].s5()
    ctx_last(1)
    og.s5()
    for r, p in ORDER:
        og.recv_sibling(r, p)
    ctx_last(2)
    ctx_last(3)
    puts = [put, *output(0, 4)]
    for x in [og, *cg]:
        x.finish()
    for c in puts:
        c.wait()


def shards(tokens, positions, norm_gain, w_query, w_key, w_value, b_query, b_key, b_value, w_out):
    rows, feats = tokens.shape
    qc, kc = w_query.shape[1], w_key.shape[1]
    wrows = w_query.shape[0]
    heads = qc // HD
    nt, ns = lax.axis_size("tensor"), lax.axis_size("seq")
    inv_freq = ROPE_BASE ** (-np.arange(HD // 2, dtype=np.float64) * 2.0 / HD)
    freq = jnp.asarray(np.concatenate([inv_freq, inv_freq])[None, :].astype(np.float32))
    hbm = pl.BlockSpec(memory_space=pltpu.HBM)
    dma = pltpu.SemaphoreType.DMA
    return pl.pallas_call(
        block_kernel,
        name="block",
        out_shape=(
            jax.ShapeDtypeStruct((rows, feats), BF16),
            jax.ShapeDtypeStruct((rows, qc), BF16),
        ),
        in_specs=[hbm] * 11,
        out_specs=(pl.BlockSpec(memory_space=pl.ANY), pl.BlockSpec(memory_space=pl.ANY)),
        scratch_shapes=[
            pltpu.VMEM((nt, 1, feats), F32),
            pltpu.VMEM((1, qc + 2 * kc), F32),
            pltpu.VMEM((1, HD), F32),
            pltpu.VMEM((rows, HD), F32),
            pltpu.VMEM((rows, HD), F32),
            pltpu.VMEM((nt, rows, feats), BF16),
            pltpu.VMEM((ns, wrows, qc + 2 * kc), BF16),
            pltpu.VMEM((rows, qc + 2 * kc), F32),
            pltpu.VMEM((rows // 2, feats), BF16),
            pltpu.VMEM((nt, 8, 128), F32),
            pltpu.VMEM((rows, 128), F32),
            pltpu.VMEM((nt, w_out.shape[0] // 8, w_out.shape[1]), BF16),
            pltpu.VMEM((ns, rows // 128, 128), jnp.int32),
            pltpu.VMEM((heads, rows, HD), BF16),
            pltpu.VMEM((ns * rows, 2 * HD), BF16),
            pltpu.VMEM((nt, 8, qc // 8, feats), BF16),
            pltpu.VMEM((rows, nt * qc), BF16),
            pltpu.VMEM((2 * ns, 1, rows // 2), F32),
            pltpu.VMEM((rows, 128), F32),
            pltpu.VMEM((heads, rows, 128), F32),
            pltpu.VMEM((heads, rows, 128), F32),
            pltpu.VMEM((heads, rows, HD), F32),
            pltpu.VMEM((rows, feats), BF16),
            dma((12,)), dma((20,)), dma((20,)), dma((18,)), dma((18,)),
            dma((7,)), dma((7,)), dma((15,)), dma((15,)), dma((16,)), dma((15,)),
            dma((36,)), dma((36,)), dma((18,)), dma((18,)), dma((32,)), dma((32,)), dma((1, 4)),
        ],
        compiler_params=pltpu.CompilerParams(
            collective_id=0, has_side_effects=True, vmem_limit_bytes=58 * 1024 * 1024
        ),
    )(
        tokens, positions.reshape(rows // 128, 128), norm_gain.reshape(nt, 1, feats), w_query, w_key, w_value,
        b_query[None, :], b_key[None, :], b_value[None, :], freq, w_out,
    )


def solution(mesh):
    in_specs = (
        P("seq", "tensor"),
        P("seq"),
        P(),
        P("seq", "tensor"),
        P("seq", "tensor"),
        P("seq", "tensor"),
        P("tensor"),
        P("tensor"),
        P("tensor"),
        P("tensor", "seq"),
    )
    out_specs = (P("seq", "tensor"), P("seq", "tensor"))
    return jax.shard_map(shards, mesh=mesh, in_specs=in_specs, out_specs=out_specs, check_vma=False)
```
